32 devices in a mesh: seq: 2 (over core), mp: 4 (over y, x), batch: 4 (over z).
Axes of the slice: x: 2, y: 2, z: 4, core: 2. Of those that a mesh axis runs over, the one named last changes fastest.
Arguments:
- queries: bfloat16 [4, 8, 4096], P('batch', 'seq', 'mp'), may hold values from -6 to 6
- keys: bfloat16 [4, 512, 1024], P('batch', 'seq', 'mp'), may hold values from -6 to 6
- values: bfloat16 [4, 512, 1024], P('batch', 'seq', 'mp'), may hold values from -6 to 6
- key_position: float32 [32, 128], replicated, may hold values from -4 to 4
- compress_keys: bfloat16 [4096, 128], replicated, may hold values from -0.2 to 0.2
- compress_values: bfloat16 [4096, 128], replicated, may hold values from -0.09375 to 0.09375
- out_proj: bfloat16 [4096, 4096], P('mp', 'seq'), may hold values from -0.09375 to 0.09375
- residual: bfloat16 [4, 8, 4096], P(None, None, 'seq'), may hold values from -6 to 6
- norm_gain: float32 [4096], replicated, may hold values from 0.25 to 1.75
- lm_head: bfloat16 [8192, 4096], P(('seq', 'mp', 'batch')), may hold values from -0.4 to 0.4
- targets: int32 [4, 8], replicated, may hold values from 0 to 8191
- lengths: int32 [4], replicated, may hold values from 128 to 512
Outputs:
- token_logprob: float32 [4, 8], P('batch', 'seq')
- rollout_score: float32 [4], P('batch')
The draws below stay inside these ranges and needn't reach their ends.
All inputs are finite; a program needn't handle non-finite values.
Results may differ from the reference program's by a relative error of at most 0.0005.
The reference program's roundings to bfloat16 on the way count: a program that leaves them out, or rounds other values in their place, can miss the bound.
Values may be sent and summed in bfloat16 or wider, within the bound.
No kernel may reach another device: no remote copies, remote signals or barrier semaphores. Data moves between devices by JAX's collectives and lax.ppermute only.
A program may use at most 64 MiB of HBM per device.

```python
import math
import jax
import jax.numpy as jnp
import numpy as np
from jax import lax

D = 4096
HEADS = 32
KV_HEADS = 8
HEAD_DIM = 128
BLOCK = 32
STRIDE = 16
SKIP = 64
LENGTH = 512
SCORED = 8
NBLK = 32
ROLLOUTS = 4
VOCAB = 8192


def labelled(key, label):
    return jax.random.fold_in(key, label)


def compress_table(key):
    fan = BLOCK * HEAD_DIM
    raw = jax.random.normal(labelled(key, 101), (fan, HEAD_DIM), jnp.float32)
    return jnp.clip(raw, -4.5, 4.5) * fan ** (-0.5)


def draw_compress_keys(key, part):
    return compress_table(key).astype(jnp.bfloat16)


def draw_keys(key, part):
    shape = (ROLLOUTS, LENGTH, KV_HEADS * HEAD_DIM)
    base = jnp.clip(jax.random.normal(labelled(key, 104), shape, jnp.float32), -6.0, 6.0)
    return base.astype(jnp.bfloat16)


def draw_queries(key, part):
    shape = (ROLLOUTS, SCORED, HEADS, HEAD_DIM)
    base = jnp.clip(jax.random.normal(labelled(key, 105), shape, jnp.float32), -6.0, 6.0)
    return base.reshape(ROLLOUTS, SCORED, HEADS * HEAD_DIM).astype(jnp.bfloat16)


def draw_residual(key, part):
    shape = (ROLLOUTS, SCORED, D)
    base = jnp.clip(jax.random.normal(labelled(key, 108), shape, jnp.float32), -6.0, 6.0)
    return base.astype(jnp.bfloat16)


def draw_lm_head(key, part):
    noise = jax.random.normal(labelled(key, 111), (VOCAB, D), jnp.float32)
    base = jnp.clip(0.047 * noise, -0.28, 0.28)
    return base.astype(jnp.bfloat16)


def touch_ends(result, key, smallest, high):
    spot = [jax.random.randint(jax.random.fold_in(key, axis), (), 0, length) for axis, length in enumerate(result.shape)]
    longest = result.shape.index(max(result.shape))
    neighbour = spot[:longest] + [(spot[longest] + 1) % result.shape[longest]] + spot[longest + 1:]
    return result.at[tuple(spot)].set(smallest).at[tuple(neighbour)].set(high)


def shard_levels(key, shape, split, smallest, largest):
    level = 1.0
    for axis_at, parts in split:
        draws = jax.random.uniform(jax.random.fold_in(jax.random.fold_in(key, 6), axis_at), (parts,), jnp.float32, smallest / len(split), largest / len(split))
        level = level * jnp.repeat(jnp.exp(draws), shape[axis_at] // parts).reshape((-1,) + (1,) * (len(shape) - 1 - axis_at))
    return level


def rank_bounds(number_of, lean):
    portions = [(1 << 20) // math.isqrt(standing ** lean) + 1 for standing in range(1, number_of + 1)]
    spread = 1 + sum(portions) // (1 << 30)
    return np.cumsum(np.array([max(1, weight // spread) for weight in portions]))


def ranked(stream_key, dims, amount, slope):
    listing = rank_bounds(amount, slope)
    ticket = jax.random.randint(jax.random.fold_in(stream_key, 1), dims, 0, int(listing[amount - 1]))
    grade = jnp.searchsorted(jnp.asarray(listing, jnp.int32), ticket, side="right")
    return jax.random.permutation(jax.random.fold_in(stream_key, 2), amount)[grade].astype(jnp.int32)


def centred(stream_key, dims, scale, bound, cuts=(), held_as=jnp.bfloat16):
    loudness = shard_levels(stream_key, dims, cuts, -0.22, 0.18) if cuts else 1.0
    result = jax.random.normal(stream_key, dims, jnp.float32) * scale * loudness
    return jnp.minimum(jnp.maximum(result, -bound), bound).astype(held_as)


def setup_inputs(seed: int = 0) -> dict:
    streams_of = jax.random.split(jax.random.key(seed), 13)
    return {
        "queries": draw_queries(jax.random.fold_in(streams_of[12], 71), 0),
        "keys": draw_keys(jax.random.fold_in(streams_of[12], 71), 0),
        "values": centred(streams_of[2], (ROLLOUTS, LENGTH, KV_HEADS * HEAD_DIM), 1.0, 6.0, ((0, 4), (1, 2), (2, 4))),
        "key_position": centred(streams_of[3], (BLOCK, HEAD_DIM), 0.7, 4.0, (), jnp.float32),
        "compress_keys": draw_compress_keys(jax.random.fold_in(streams_of[12], 71), 0),
        "compress_values": centred(streams_of[5], (BLOCK * HEAD_DIM, HEAD_DIM), (BLOCK * HEAD_DIM) ** -0.5, 0.09375),
        "out_proj": centred(streams_of[6], (HEADS * HEAD_DIM, D), (HEADS * HEAD_DIM) ** -0.5, 0.09375, ((0, 4), (1, 2))),
        "residual": draw_residual(jax.random.fold_in(streams_of[12], 71), 0),
        "norm_gain": jnp.clip(1.0 + 0.15 * jax.random.normal(streams_of[8], (D,), jnp.float32), 0.25, 1.75),
        "lm_head": draw_lm_head(jax.random.fold_in(streams_of[12], 71), 0),
        "targets": touch_ends(ranked(streams_of[10], (ROLLOUTS, SCORED), VOCAB, 2), jax.random.fold_in(streams_of[10], 3), 0, VOCAB - 1).astype(jnp.int32),
        "lengths": touch_ends(jax.random.randint(streams_of[11], (ROLLOUTS,), LENGTH // 4, LENGTH + 1), jax.random.fold_in(streams_of[11], 1), LENGTH // 4, LENGTH).astype(jnp.int32),
    }


def compress(rows, position, weight):
    total = rows.shape[0]
    shaped = rows.reshape(total, KV_HEADS, HEAD_DIM)
    padded = jnp.concatenate([shaped, jnp.zeros((STRIDE, KV_HEADS, HEAD_DIM), shaped.dtype)], 0)
    first = padded[:total].reshape(total // STRIDE, STRIDE, KV_HEADS, HEAD_DIM)
    second = padded[STRIDE:].reshape(total // STRIDE, STRIDE, KV_HEADS, HEAD_DIM)
    blocks = jnp.concatenate([first, second], 1)
    blocks = (blocks.astype(jnp.float32) + position[None, :, None, :]).astype(jnp.bfloat16)
    mapped = jnp.einsum('bjhd,jde->bhe', blocks.astype(jnp.float32), weight.reshape(BLOCK, HEAD_DIM, HEAD_DIM).astype(jnp.float32))
    return mapped.astype(jnp.bfloat16)

def score_rollout(query_rows, key_rows, value_rows, residual_rows, target_rows, key_position, compress_keys, compress_values, out_proj, norm_gain, lm_head):
    ckey = compress(key_rows, key_position, compress_keys)
    cvalue = compress(value_rows, key_position, compress_values)
    group = HEADS // KV_HEADS
    query = query_rows.reshape(SCORED, KV_HEADS, group, HEAD_DIM).astype(jnp.float32)
    scores = jnp.einsum('qhgd,bhd->qhgb', query, ckey.astype(jnp.float32)) * (1.0 / math.sqrt(HEAD_DIM))
    limit = jnp.arange(SCORED, dtype=jnp.int32) * SKIP // STRIDE
    visible = (jnp.arange(NBLK, dtype=jnp.int32)[None, :] <= limit[:, None])[:, None, None, :]
    scores = jnp.where(visible, scores, -1e+30)
    peak = lax.optimization_barrier(jnp.max(scores, -1, keepdims=True))
    weights = jnp.where(visible, jnp.exp(scores - peak), 0.0)
    probs = (weights / lax.optimization_barrier(jnp.sum(weights, -1, keepdims=True))).astype(jnp.bfloat16)
    attended = jnp.einsum('qhgb,bhd->qhgd', probs.astype(jnp.float32), cvalue.astype(jnp.float32))
    attended = attended.astype(jnp.bfloat16).reshape(SCORED, HEADS * HEAD_DIM)
    hidden = (residual_rows.astype(jnp.float32) + jnp.dot(attended, out_proj, preferred_element_type=jnp.float32)).astype(jnp.bfloat16)
    widened = hidden.astype(jnp.float32)
    meansq = lax.optimization_barrier(jnp.mean(widened * widened, -1, keepdims=True))
    normed = (widened * lax.rsqrt(meansq + 1e-05) * norm_gain).astype(jnp.bfloat16)
    logits = jnp.dot(normed, lm_head.T, preferred_element_type=jnp.float32)
    top = lax.optimization_barrier(jnp.max(logits, -1, keepdims=True))
    logsum = top[:, 0] + jnp.log(lax.optimization_barrier(jnp.sum(jnp.exp(logits - top), -1)))
    picked = jnp.take_along_axis(logits, target_rows[:, None], 1)[:, 0]
    return picked - logsum

def reference(queries, keys, values, key_position, compress_keys, compress_values, out_proj, residual, norm_gain, lm_head, targets, lengths):

    def one(items):
        return score_rollout(items[0], items[1], items[2], items[3], items[4], key_position, compress_keys, compress_values, out_proj, norm_gain, lm_head)
    token_logprob = lax.map(one, (queries, keys, values, residual, targets))
    spots = jnp.arange(SCORED, dtype=jnp.int32) * SKIP + BLOCK - 1
    valid = (spots[None, :] < lengths[:, None]).astype(jnp.float32)
    count = jnp.sum(valid)
    rollout_score = lax.optimization_barrier(jnp.sum(valid * token_logprob, 1)) / count
    return (token_logprob, rollout_score)
```

```python
import math

import jax
import jax.numpy as jnp
from jax import lax
from jax.sharding import PartitionSpec as P

HEAD_DIM = 128
BLOCK = 32
STRIDE = 16


def from_behind(block, axis, distance):
    devices = range(lax.axis_size(axis))
    route = [(i - distance, i) for i in devices if i - distance in devices]
    return lax.ppermute(block, axis, route)


def compress_rows(rows, following, position, weight):
    extended = jnp.concatenate([rows, following], 0)
    count = rows.shape[0] // STRIDE
    heads = rows.shape[1] // HEAD_DIM
    shaped = extended.reshape(count + 1, STRIDE, heads, HEAD_DIM)
    blocks = jnp.concatenate([shaped[:-1], shaped[1:]], 1)
    blocks = (blocks.astype(jnp.float32) + position[None, :, None, :]).astype(jnp.bfloat16)
    mapped = jnp.einsum(
        "bjhd,jde->bhe",
        blocks,
        weight.reshape(BLOCK, HEAD_DIM, HEAD_DIM),
        preferred_element_type=jnp.float32,
    )
    return mapped.astype(jnp.bfloat16).reshape(count, heads * HEAD_DIM)


def normalize(hidden, gain):
    widened = hidden.astype(jnp.float32)
    meansq = jnp.mean(widened * widened, -1, keepdims=True)
    return (widened * lax.rsqrt(meansq + 1e-05) * gain).astype(jnp.bfloat16)


def vocab_logits(normed, rows):
    return lax.dot_general(
        normed, rows, (((1,), (1,)), ((), ())), preferred_element_type=jnp.float32
    )


def picked_logit(logits, offset, wanted):
    columns = offset + jnp.arange(logits.shape[1], dtype=jnp.int32)
    hits = columns[None, :] == wanted[:, None]
    return jnp.sum(jnp.where(hits, logits, 0.0), 1)

DIRECT = 4
SPREAD = 64


def pairs(axis, distance):
    return [(i, i ^ distance) for i in range(lax.axis_size(axis))]


def direct(axis):
    count = lax.axis_size(axis)
    return count <= DIRECT and count & (count - 1) == 0


def exchange(block, axis):
    return [block] + [
        lax.ppermute(block, axis, pairs(axis, distance))
        for distance in range(1, lax.axis_size(axis))
    ]


def by_position(blocks, axis):
    place = lax.axis_index(axis)
    step = 1
    while step < len(blocks):
        odd = (place // step) % 2 == 1
        blocks = [jnp.where(odd, blocks[i ^ step], blocks[i]) for i in range(len(blocks))]
        step *= 2
    return blocks


def pair_sum(blocks):
    while len(blocks) > 1:
        blocks = [blocks[i] + blocks[i + 1] for i in range(0, len(blocks), 2)]
    return blocks[0]


def sum_over(part, axis):
    if direct(axis):
        return pair_sum(exchange(part, axis))
    return lax.psum(part, axis)


def gather_over(block, axis, dimension):
    if direct(axis):
        return jnp.concatenate(by_position(exchange(block, axis), axis), dimension)
    return lax.all_gather(block, axis, axis=dimension, tiled=True)


def attend(query, all_keys, all_values, first, skip):
    count = query.shape[0]
    blocks = all_keys.shape[0]
    scores = jnp.einsum("qhgd,bhd->qhgb", query, all_keys, preferred_element_type=jnp.float32) * (
        1.0 / math.sqrt(HEAD_DIM)
    )
    index = first + jnp.arange(count, dtype=jnp.int32)
    limit = index * skip // STRIDE
    visible = (jnp.arange(blocks, dtype=jnp.int32)[None, :] <= limit[:, None])[:, None, None, :]
    scores = jnp.where(visible, scores, -1e30)
    peak = jnp.max(scores, -1, keepdims=True)
    weights = jnp.where(visible, jnp.exp(scores - peak), 0.0)
    probs = (weights / jnp.sum(weights, -1, keepdims=True)).astype(jnp.bfloat16)
    attended = jnp.einsum("qhgb,bhd->qhgd", probs, all_values, preferred_element_type=jnp.float32)
    return attended.astype(jnp.bfloat16).reshape(count, -1)


def attend_whole(queries, keys, values, key_position, compress_keys, compress_values, skip):
    rows = gather_over(keys, "seq", 0)
    vals = gather_over(values, "seq", 0)
    query = gather_over(queries, "seq", 0)
    none = jnp.zeros((STRIDE, rows.shape[1]), rows.dtype)
    comp_keys = compress_rows(rows, none, key_position, compress_keys)
    comp_values = compress_rows(vals, none, key_position, compress_values)
    heads = rows.shape[1] // HEAD_DIM
    group = query.shape[1] // HEAD_DIM // heads
    return attend(
        query.reshape(-1, heads, group, HEAD_DIM),
        comp_keys.reshape(-1, heads, HEAD_DIM),
        comp_values.reshape(-1, heads, HEAD_DIM),
        0,
        skip,
    )


def attend_segments(queries, keys, values, key_position, compress_keys, compress_values, skip):
    following = from_behind((keys[:STRIDE], values[:STRIDE]), "seq", -1)
    comp_keys = compress_rows(keys, following[0], key_position, compress_keys)
    comp_values = compress_rows(values, following[1], key_position, compress_values)
    every = lax.all_gather(jnp.stack([comp_keys, comp_values], 0), "seq", axis=1, tiled=True)
    heads = keys.shape[1] // HEAD_DIM
    group = queries.shape[1] // HEAD_DIM // heads
    blocks = every.shape[1]
    attended = attend(
        queries.reshape(-1, heads, group, HEAD_DIM),
        every[0].reshape(blocks, heads, HEAD_DIM),
        every[1].reshape(blocks, heads, HEAD_DIM),
        lax.axis_index("seq") * queries.shape[0],
        skip,
    )
    return lax.all_gather(attended, "seq", axis=0, tiled=True)


EVERY = ("seq", "mp", "batch")


def log_probs(logits, wanted, offset):
    picked = picked_logit(logits, offset, wanted)
    local_top = jnp.max(logits, 1)
    devices = lax.axis_size(EVERY)
    if devices > SPREAD:
        top = lax.pmax(local_top, EVERY)
        local_sum = jnp.sum(jnp.exp(logits - top[:, None]), 1)
        total, target_logit = lax.psum((local_sum, picked), EVERY)
        return target_logit - (top + jnp.log(total))
    local_sum = jnp.sum(jnp.exp(logits - local_top[:, None]), 1)
    mine = jnp.concatenate([local_top, local_sum, picked], 0)
    sent = jnp.broadcast_to(mine[None, :], (devices, mine.shape[0]))
    tops, sums, hits = jnp.split(lax.all_to_all(sent, EVERY, 0, 0, tiled=True), 3, 1)
    top = jnp.max(tops, 0)
    total = jnp.sum(sums * jnp.exp(tops - top[None, :]), 0)
    return jnp.sum(hits, 0) - (top + jnp.log(total))


def body(
    queries,
    keys,
    values,
    key_position,
    compress_keys,
    compress_values,
    out_proj,
    residual,
    norm_gain,
    lm_head,
    targets,
    lengths,
):
    seq_pos = lax.axis_index("seq")
    batch_pos = lax.axis_index("batch")
    qcount = queries.shape[1]
    skip = keys.shape[1] // qcount
    rollouts, scored = targets.shape
    attention = attend_whole if direct("seq") else attend_segments
    attended = attention(
        queries[0], keys[0], values[0], key_position, compress_keys, compress_values, skip
    )
    part = jnp.dot(attended, out_proj, preferred_element_type=jnp.float32)
    summed = sum_over(part, "mp")
    hidden = (residual[batch_pos].astype(jnp.float32) + summed).astype(jnp.bfloat16)
    whole = gather_over(gather_over(hidden, "batch", 0), "seq", 1)
    normed = normalize(whole, norm_gain)
    logits = vocab_logits(normed, lm_head)
    offset = lax.axis_index(EVERY) * lm_head.shape[0]
    by_rollout = log_probs(logits, targets.reshape(-1), offset).reshape(rollouts, scored)
    spots = jnp.arange(scored, dtype=jnp.int32) * skip + BLOCK - 1
    valid = (spots[None, :] < lengths[:, None]).astype(jnp.float32)
    count = jnp.sum(valid)
    token_logprob = lax.dynamic_slice(by_rollout, (batch_pos, seq_pos * qcount), (1, qcount))
    sums = jnp.sum(valid * by_rollout, 1) / count
    rollout_score = sums[batch_pos][None]
    return (token_logprob, rollout_score)


def solution(mesh):
    in_specs = (
        P("batch", "seq", "mp"),
        P("batch", "seq", "mp"),
        P("batch", "seq", "mp"),
        P(),
        P(),
        P(),
        P("mp", "seq"),
        P(None, None, "seq"),
        P(),
        P(("seq", "mp", "batch"), None),
        P(),
        P(),
    )
    out_specs = (P("batch", "seq"), P("batch"))
    return jax.shard_map(body, mesh=mesh, in_specs=in_specs, out_specs=out_specs, check_vma=False)
```

```python
import functools
import math

import jax
import jax.numpy as jnp
from jax import lax
from jax.experimental import pallas as pl
from jax.experimental.pallas import tpu as pltpu
from jax.sharding import PartitionSpec as P

HEAD_DIM = 128
BLOCK = 32
STRIDE = 16


def from_behind(block, axis, distance):
    devices = range(lax.axis_size(axis))
    route = [(i - distance, i) for i in devices if i - distance in devices]
    return lax.ppermute(block, axis, route)


def compress_rows(rows, following, position, weight):
    extended = jnp.concatenate([rows, following], 0)
    count = rows.shape[0] // STRIDE
    heads = rows.shape[1] // HEAD_DIM
    shaped = extended.reshape(count + 1, STRIDE, heads, HEAD_DIM)
    blocks = jnp.concatenate([shaped[:-1], shaped[1:]], 1)
    blocks = (blocks.astype(jnp.float32) + position[None, :, None, :]).astype(jnp.bfloat16)
    mapped = jnp.einsum(
        "bjhd,jde->bhe",
        blocks,
        weight.reshape(BLOCK, HEAD_DIM, HEAD_DIM),
        preferred_element_type=jnp.float32,
    )
    return mapped.astype(jnp.bfloat16).reshape(count, heads * HEAD_DIM)


def normalize(hidden, gain):
    widened = hidden.astype(jnp.float32)
    meansq = jnp.mean(widened * widened, -1, keepdims=True)
    return (widened * lax.rsqrt(meansq + 1e-05) * gain).astype(jnp.bfloat16)


def vocab_logits(normed, rows):
    return lax.dot_general(
        normed, rows, (((1,), (1,)), ((), ())), preferred_element_type=jnp.float32
    )


def picked_logit(logits, offset, wanted):
    columns = offset + jnp.arange(logits.shape[1], dtype=jnp.int32)
    hits = columns[None, :] == wanted[:, None]
    return jnp.sum(jnp.where(hits, logits, 0.0), 1)

DIRECT = 4
SPREAD = 64


def pairs(axis, distance):
    return [(i, i ^ distance) for i in range(lax.axis_size(axis))]


def direct(axis):
    count = lax.axis_size(axis)
    return count <= DIRECT and count & (count - 1) == 0


def exchange(block, axis):
    return [block] + [
        lax.ppermute(block, axis, pairs(axis, distance))
        for distance in range(1, lax.axis_size(axis))
    ]


def by_position(blocks, axis):
    place = lax.axis_index(axis)
    step = 1
    while step < len(blocks):
        odd = (place // step) % 2 == 1
        blocks = [jnp.where(odd, blocks[i ^ step], blocks[i]) for i in range(len(blocks))]
        step *= 2
    return blocks


def pair_sum(blocks):
    while len(blocks) > 1:
        blocks = [blocks[i] + blocks[i + 1] for i in range(0, len(blocks), 2)]
    return blocks[0]


def sum_over(part, axis):
    if direct(axis):
        return pair_sum(exchange(part, axis))
    return lax.psum(part, axis)


def gather_over(block, axis, dimension):
    if direct(axis):
        return jnp.concatenate(by_position(exchange(block, axis), axis), dimension)
    return lax.all_gather(block, axis, axis=dimension, tiled=True)


def attend(query, all_keys, all_values, first, skip):
    count = query.shape[0]
    blocks = all_keys.shape[0]
    scores = jnp.einsum("qhgd,bhd->qhgb", query, all_keys, preferred_element_type=jnp.float32) * (
        1.0 / math.sqrt(HEAD_DIM)
    )
    index = first + jnp.arange(count, dtype=jnp.int32)
    limit = index * skip // STRIDE
    visible = (jnp.arange(blocks, dtype=jnp.int32)[None, :] <= limit[:, None])[:, None, None, :]
    scores = jnp.where(visible, scores, -1e30)
    peak = jnp.max(scores, -1, keepdims=True)
    weights = jnp.where(visible, jnp.exp(scores - peak), 0.0)
    probs = (weights / jnp.sum(weights, -1, keepdims=True)).astype(jnp.bfloat16)
    attended = jnp.einsum("qhgb,bhd->qhgd", probs, all_values, preferred_element_type=jnp.float32)
    return attended.astype(jnp.bfloat16).reshape(count, -1)


def attend_whole(queries, keys, values, key_position, compress_keys, compress_values, skip):
    rows = gather_over(keys, "seq", 0)
    vals = gather_over(values, "seq", 0)
    query = gather_over(queries, "seq", 0)
    none = jnp.zeros((STRIDE, rows.shape[1]), rows.dtype)
    comp_keys = compress_rows(rows, none, key_position, compress_keys)
    comp_values = compress_rows(vals, none, key_position, compress_values)
    heads = rows.shape[1] // HEAD_DIM
    group = query.shape[1] // HEAD_DIM // heads
    return attend(
        query.reshape(-1, heads, group, HEAD_DIM),
        comp_keys.reshape(-1, heads, HEAD_DIM),
        comp_values.reshape(-1, heads, HEAD_DIM),
        0,
        skip,
    )


def attend_segments(queries, keys, values, key_position, compress_keys, compress_values, skip):
    following = from_behind((keys[:STRIDE], values[:STRIDE]), "seq", -1)
    comp_keys = compress_rows(keys, following[0], key_position, compress_keys)
    comp_values = compress_rows(values, following[1], key_position, compress_values)
    every = lax.all_gather(jnp.stack([comp_keys, comp_values], 0), "seq", axis=1, tiled=True)
    heads = keys.shape[1] // HEAD_DIM
    group = queries.shape[1] // HEAD_DIM // heads
    blocks = every.shape[1]
    attended = attend(
        queries.reshape(-1, heads, group, HEAD_DIM),
        every[0].reshape(blocks, heads, HEAD_DIM),
        every[1].reshape(blocks, heads, HEAD_DIM),
        lax.axis_index("seq") * queries.shape[0],
        skip,
    )
    return lax.all_gather(attended, "seq", axis=0, tiled=True)


EVERY = ("seq", "mp", "batch")


def log_probs(logits, wanted, offset):
    picked = picked_logit(logits, offset, wanted)
    local_top = jnp.max(logits, 1)
    devices = lax.axis_size(EVERY)
    if devices > SPREAD:
        top = lax.pmax(local_top, EVERY)
        local_sum = jnp.sum(jnp.exp(logits - top[:, None]), 1)
        total, target_logit = lax.psum((local_sum, picked), EVERY)
        return target_logit - (top + jnp.log(total))
    local_sum = jnp.sum(jnp.exp(logits - local_top[:, None]), 1)
    mine = jnp.concatenate([local_top, local_sum, picked], 0)
    sent = jnp.broadcast_to(mine[None, :], (devices, mine.shape[0]))
    tops, sums, hits = jnp.split(lax.all_to_all(sent, EVERY, 0, 0, tiled=True), 3, 1)
    top = jnp.max(tops, 0)
    total = jnp.sum(sums * jnp.exp(tops - top[None, :]), 0)
    return jnp.sum(hits, 0) - (top + jnp.log(total))


def large_mesh(
    queries,
    keys,
    values,
    key_position,
    compress_keys,
    compress_values,
    out_proj,
    residual,
    norm_gain,
    lm_head,
    targets,
    lengths,
):
    seq_pos = lax.axis_index("seq")
    batch_pos = lax.axis_index("batch")
    qcount = queries.shape[1]
    skip = keys.shape[1] // qcount
    rollouts, scored = targets.shape
    attention = attend_whole if direct("seq") else attend_segments
    attended = attention(
        queries[0], keys[0], values[0], key_position, compress_keys, compress_values, skip
    )
    part = jnp.dot(attended, out_proj, preferred_element_type=jnp.float32)
    summed = sum_over(part, "mp")
    hidden = (residual[batch_pos].astype(jnp.float32) + summed).astype(jnp.bfloat16)
    whole = gather_over(gather_over(hidden, "batch", 0), "seq", 1)
    normed = normalize(whole, norm_gain)
    logits = vocab_logits(normed, lm_head)
    offset = lax.axis_index(EVERY) * lm_head.shape[0]
    by_rollout = log_probs(logits, targets.reshape(-1), offset).reshape(rollouts, scored)
    spots = jnp.arange(scored, dtype=jnp.int32) * skip + BLOCK - 1
    valid = (spots[None, :] < lengths[:, None]).astype(jnp.float32)
    count = jnp.sum(valid)
    token_logprob = lax.dynamic_slice(by_rollout, (batch_pos, seq_pos * qcount), (1, qcount))
    sums = jnp.sum(valid * by_rollout, 1) / count
    rollout_score = sums[batch_pos][None]
    return (token_logprob, rollout_score)


VMEM = pl.BlockSpec(memory_space=pltpu.VMEM)
SMEM = pl.BlockSpec(memory_space=pltpu.SMEM)
NT = (((1,), (1,)), ((), ()))
LANES = 128
FILL = 20_000_000_000


def swap(block):
    return lax.ppermute(block, "seq", [(0, 1), (1, 0)])


def crossed(block, axis, distance):
    count = lax.axis_size(axis)
    route = [
        (core * count + i, (1 - core) * count + (i ^ distance))
        for core in range(2)
        for i in range(count)
    ]
    return lax.ppermute(block, ("seq", axis), route)


def compress_all(rows, position, weight):
    blocks = rows.shape[1] // STRIDE - 1
    total = None
    for first in range(0, BLOCK, 2):
        sides = []
        for i in (first, first + 1):
            offset = position[i : i + 1, :]
            sides.append(
                jnp.concatenate(
                    [
                        rows[head, pl.ds(i, blocks, stride=STRIDE), :] + offset
                        for head in range(rows.shape[0])
                    ],
                    0,
                )
            )
        left = jnp.concatenate(sides, 1).astype(jnp.bfloat16)
        right = weight[first * HEAD_DIM : (first + 2) * HEAD_DIM, :]
        term = jnp.dot(left, right, preferred_element_type=jnp.float32)
        total = term if total is None else total + term
    total = total.astype(jnp.bfloat16)
    return [total[h * blocks : (h + 1) * blocks, :] for h in range(rows.shape[0])]


def attention_kernel(
    skip,
    k_mine,
    k_other,
    v_mine,
    v_other,
    q_mine,
    q_other,
    position,
    weight_k,
    weight_v,
    out_proj,
    base,
    part,
    k_rows,
    v_rows,
    q_rows,
):
    core = lax.axis_index("seq")
    length, width = k_mine.shape
    heads = width // HEAD_DIM
    for rows, mine, other in ((k_rows, k_mine, k_other), (v_rows, v_mine, v_other)):
        for place, half in ((core, mine), (1 - core, other)):
            where = pl.ds(pl.multiple_of(place * length, length), length)
            for head in range(heads):
                rows[head, where, :] = half[:, head * HEAD_DIM : (head + 1) * HEAD_DIM].astype(
                    jnp.float32
                )
        rows[:, 2 * length :, :] = jnp.zeros((heads, STRIDE, HEAD_DIM), jnp.float32)
    few = q_mine.shape[0]
    mine = q_mine[...].astype(jnp.float32)
    other = q_other[...].astype(jnp.float32)
    q_rows[:few, :] = jnp.where(core == 0, mine, other)
    q_rows[few:, :] = jnp.where(core == 0, other, mine)
    count = 2 * few
    keys = compress_all(k_rows, position, weight_k)
    values = compress_all(v_rows, position, weight_v)
    group = q_rows.shape[1] // HEAD_DIM // heads
    blocks = keys[0].shape[0]
    row = lax.broadcasted_iota(jnp.int32, (group * count, blocks), 0)
    column = lax.broadcasted_iota(jnp.int32, (group * count, blocks), 1)
    visible = column <= row % count * skip // STRIDE
    lanes = []
    for head in range(heads):
        query = jnp.concatenate(
            [
                q_rows[:, (head * group + g) * HEAD_DIM : (head * group + g + 1) * HEAD_DIM]
                for g in range(group)
            ],
            0,
        ).astype(jnp.bfloat16)
        scores = lax.dot_general(query, keys[head], NT, preferred_element_type=jnp.float32)
        scores = jnp.where(visible, scores * (1.0 / math.sqrt(HEAD_DIM)), -1e30)
        peak = jnp.max(scores, -1, keepdims=True)
        weights = jnp.where(visible, jnp.exp(scores - peak), 0.0)
        probs = (weights / jnp.sum(weights, -1, keepdims=True)).astype(jnp.bfloat16)
        attended = jnp.dot(probs, values[head], preferred_element_type=jnp.float32)
        attended = attended.astype(jnp.bfloat16).astype(jnp.float32)
        lanes += [attended[g * count : (g + 1) * count, :] for g in range(group)]
    attended = jnp.concatenate(lanes, 1).astype(jnp.bfloat16)
    product = jnp.dot(attended, out_proj[...], preferred_element_type=jnp.float32)
    part[...] = product + base[...]


def residual_kernel(residual, base):
    mine = residual[lax.axis_index("batch")].astype(jnp.float32)
    base[...] = jnp.where(lax.axis_index("mp") == 0, mine, 0.0)


def residual_once(residual):
    return pl.pallas_call(
        residual_kernel,
        out_shape=jax.ShapeDtypeStruct(residual.shape[1:], jnp.float32),
        in_specs=[VMEM],
        out_specs=VMEM,
        compiler_params=pltpu.CompilerParams(vmem_limit_bytes=4 << 20),
        cost_estimate=pl.CostEstimate(flops=FILL, bytes_accessed=2 * residual.size, transcendentals=0),
        name="residual",
    )(residual)


def attention_part(
    keys, values, queries, key_position, compress_keys, compress_values, out_proj, residual, skip
):
    length, width = keys.shape
    heads = width // HEAD_DIM
    count = 2 * queries.shape[0]
    rows = pltpu.VMEM((heads, 2 * length + STRIDE, HEAD_DIM), jnp.float32)
    return pl.pallas_call(
        functools.partial(attention_kernel, skip),
        out_shape=jax.ShapeDtypeStruct((count, out_proj.shape[1]), jnp.float32),
        in_specs=[VMEM] * 11,
        out_specs=VMEM,
        scratch_shapes=[rows, rows, pltpu.VMEM((count, queries.shape[1]), jnp.float32)],
        compiler_params=pltpu.CompilerParams(vmem_limit_bytes=24 << 20),
        cost_estimate=pl.CostEstimate(
            flops=2 * count * out_proj.size + 8 * length * width * HEAD_DIM * 2,
            bytes_accessed=2 * (out_proj.size + compress_keys.size + compress_values.size),
            transcendentals=count * 1024,
        ),
        name="attention",
    )(
        keys,
        swap(keys),
        values,
        swap(values),
        queries,
        swap(queries),
        key_position,
        compress_keys,
        compress_values,
        out_proj,
        residual_once(residual),
    )


def logits_kernel(batch, *refs):
    near, far = refs[:batch], refs[batch : 2 * batch]
    gain, lm_head, wanted, sent = refs[2 * batch :]
    core = lax.axis_index("seq")
    blocks = []
    for n, f in zip(near, far):
        n = n[...].astype(jnp.float32)
        f = f[...].astype(jnp.float32)
        blocks.append(
            jnp.concatenate([jnp.where(core == 0, n, f), jnp.where(core == 0, f, n)], 1)
        )
    hidden = jnp.concatenate(by_position(blocks, "batch"), 0)
    meansq = jnp.mean(hidden * hidden, -1, keepdims=True)
    normed = (hidden * lax.rsqrt(meansq + 1e-05) * gain[...]).astype(jnp.bfloat16)
    logits = lax.dot_general(lm_head[...], normed, NT, preferred_element_type=jnp.float32)
    share, rows = logits.shape
    offset = device_index() * share
    ids = offset + lax.broadcasted_iota(jnp.int32, (share, rows), 0)
    top = jnp.max(logits, 0, keepdims=True)
    total = jnp.sum(jnp.exp(logits - top), 0, keepdims=True)
    picked = jnp.sum(jnp.where(ids == wanted[...], logits, 0.0), 0, keepdims=True)
    pad = jnp.zeros((1, sent.shape[1] - 3 * rows), jnp.float32)
    sent[...] = jnp.broadcast_to(jnp.concatenate([top, total, picked, pad], 1), sent.shape)


def device_index():
    index = 0
    for axis in EVERY:
        index = index * lax.axis_size(axis) + lax.axis_index(axis)
    return index


def share_statistics(near, far, norm_gain, lm_head, wanted):
    rows = wanted.shape[1]
    across = -(-3 * rows // LANES) * LANES
    return pl.pallas_call(
        functools.partial(logits_kernel, len(near)),
        out_shape=jax.ShapeDtypeStruct((lax.axis_size(EVERY), across), jnp.float32),
        in_specs=[VMEM] * (2 * len(near) + 3),
        out_specs=VMEM,
        compiler_params=pltpu.CompilerParams(vmem_limit_bytes=24 << 20),
        cost_estimate=pl.CostEstimate(
            flops=2 * rows * lm_head.size, bytes_accessed=2 * lm_head.size, transcendentals=rows * 1024
        ),
        name="statistics",
    )(*near, *far, norm_gain.reshape(1, -1), lm_head, wanted)


def score_kernel(skip, scored, few, got, lengths, token, score):
    rows = lengths.shape[0] * scored
    tops = got[:, :rows]
    top = jnp.max(tops, 0, keepdims=True)
    total = jnp.sum(got[:, rows : 2 * rows] * jnp.exp(tops - top), 0, keepdims=True)
    picked = jnp.sum(got[:, 2 * rows : 3 * rows], 0, keepdims=True)
    logprob = picked - (top + jnp.log(total))
    index = lax.broadcasted_iota(jnp.int32, (1, rows), 1)
    spot = index % scored * skip + BLOCK - 1
    reach = jnp.zeros((1, rows), jnp.int32)
    for rollout in range(lengths.shape[0]):
        reach = jnp.where(index // scored == rollout, lengths[rollout], reach)
    valid = (spot < reach).astype(jnp.float32)
    count = jnp.sum(valid, 1, keepdims=True)
    batch = lax.axis_index("batch")
    mine = jnp.where(index // scored == batch, valid * logprob, 0.0)
    score[...] = jnp.sum(mine, 1, keepdims=True) / count
    start = batch * scored + lax.axis_index("seq") * few
    row = lax.broadcasted_iota(jnp.int32, (rows, few), 0)
    column = lax.broadcasted_iota(jnp.int32, (rows, few), 1)
    out = jnp.zeros((1, few), jnp.float32)
    lane = lax.broadcasted_iota(jnp.int32, (1, few), 1)
    for j in range(few):
        value = jnp.sum(jnp.where(index == start + j, logprob, 0.0), 1, keepdims=True)
        out = jnp.where(lane == j, value, out)
    token[...] = out


def final_scores(got, lengths, scored, few, skip):
    token, score = pl.pallas_call(
        functools.partial(score_kernel, skip, scored, few),
        out_shape=(
            jax.ShapeDtypeStruct((1, few), jnp.float32),
            jax.ShapeDtypeStruct((1, 1), jnp.float32),
        ),
        in_specs=[VMEM, SMEM],
        out_specs=(VMEM, VMEM),
        name="scores",
    )(got, lengths)
    return token, score.reshape(1)


def small_mesh(
    queries,
    keys,
    values,
    key_position,
    compress_keys,
    compress_values,
    out_proj,
    residual,
    norm_gain,
    lm_head,
    targets,
    lengths,
):
    few = queries.shape[1]
    skip = keys.shape[1] // few
    part = attention_part(
        keys[0],
        values[0],
        queries[0],
        key_position,
        compress_keys,
        compress_values,
        out_proj,
        residual,
        skip,
    )
    parts = [swap(part)] + [crossed(part, "mp", d) for d in range(1, lax.axis_size("mp"))]
    far = [pair_sum(parts).astype(jnp.bfloat16)]
    near = [crossed(far[0], "batch", d) for d in range(1, lax.axis_size("batch"))]
    far += [swap(block) for block in near]
    near = [swap(far[0])] + near
    sent = share_statistics(near, far, norm_gain, lm_head, targets.reshape(1, -1))
    got = lax.all_to_all(sent, EVERY, 0, 0, tiled=True)
    return final_scores(got, lengths, targets.shape[1], few, skip)


def body(*arrays):
    small = (
        lax.axis_size("seq") == 2
        and direct("mp")
        and direct("batch")
        and lax.axis_size(EVERY) <= SPREAD
    )
    return small_mesh(*arrays) if small else large_mesh(*arrays)


def solution(mesh):
    in_specs = (
        P("batch", "seq", "mp"),
        P("batch", "seq", "mp"),
        P("batch", "seq", "mp"),
        P(),
        P(),
        P(),
        P("mp", "seq"),
        P(None, None, "seq"),
        P(),
        P(("seq", "mp", "batch"), None),
        P(),
        P(),
    )
    out_specs = (P("batch", "seq"), P("batch"))
    return jax.shard_map(body, mesh=mesh, in_specs=in_specs, out_specs=out_specs, check_vma=False)
```

```python
import functools
import math

import jax
import jax.numpy as jnp
from jax import lax
from jax.experimental import pallas as pl
from jax.experimental.pallas import tpu as pltpu
from jax.sharding import PartitionSpec as P


HEAD_DIM = 128
BLOCK = 32
STRIDE = 16


def from_behind(block, axis, distance):
    devices = range(lax.axis_size(axis))
    route = [(i - distance, i) for i in devices if i - distance in devices]
    return lax.ppermute(block, axis, route)


def compress_rows(rows, following, position, weight):
    extended = jnp.concatenate([rows, following], 0)
    count = rows.shape[0] // STRIDE
    heads = rows.shape[1] // HEAD_DIM
    shaped = extended.reshape(count + 1, STRIDE, heads, HEAD_DIM)
    blocks = jnp.concatenate([shaped[:-1], shaped[1:]], 1)
    blocks = (blocks.astype(jnp.float32) + position[None, :, None, :]).astype(jnp.bfloat16)
    mapped = jnp.einsum(
        "bjhd,jde->bhe",
        blocks,
        weight.reshape(BLOCK, HEAD_DIM, HEAD_DIM),
        preferred_element_type=jnp.float32,
    )
    return mapped.astype(jnp.bfloat16).reshape(count, heads * HEAD_DIM)


def normalize(hidden, gain):
    widened = hidden.astype(jnp.float32)
    meansq = jnp.mean(widened * widened, -1, keepdims=True)
    return (widened * lax.rsqrt(meansq + 1e-05) * gain).astype(jnp.bfloat16)


def vocab_logits(normed, rows):
    return lax.dot_general(
        normed, rows, (((1,), (1,)), ((), ())), preferred_element_type=jnp.float32
    )


def picked_logit(logits, offset, wanted):
    columns = offset + jnp.arange(logits.shape[1], dtype=jnp.int32)
    hits = columns[None, :] == wanted[:, None]
    return jnp.sum(jnp.where(hits, logits, 0.0), 1)


DIRECT = 4
SPREAD = 64


def pairs(axis, distance):
    return [(i, i ^ distance) for i in range(lax.axis_size(axis))]


def direct(axis):
    count = lax.axis_size(axis)
    return count <= DIRECT and count & (count - 1) == 0


def exchange(block, axis):
    return [block] + [
        lax.ppermute(block, axis, pairs(axis, distance))
        for distance in range(1, lax.axis_size(axis))
    ]


def by_position(blocks, axis):
    place = lax.axis_index(axis)
    step = 1
    while step < len(blocks):
        odd = (place // step) % 2 == 1
        blocks = [jnp.where(odd, blocks[i ^ step], blocks[i]) for i in range(len(blocks))]
        step *= 2
    return blocks


def pair_sum(blocks):
    while len(blocks) > 1:
        blocks = [blocks[i] + blocks[i + 1] for i in range(0, len(blocks), 2)]
    return blocks[0]


def sum_over(part, axis):
    if direct(axis):
        return pair_sum(exchange(part, axis))
    return lax.psum(part, axis)


def gather_over(block, axis, dimension):
    if direct(axis):
        return jnp.concatenate(by_position(exchange(block, axis), axis), dimension)
    return lax.all_gather(block, axis, axis=dimension, tiled=True)


def attend(query, all_keys, all_values, first, skip):
    count = query.shape[0]
    blocks = all_keys.shape[0]
    scores = jnp.einsum("qhgd,bhd->qhgb", query, all_keys, preferred_element_type=jnp.float32) * (
        1.0 / math.sqrt(HEAD_DIM)
    )
    index = first + jnp.arange(count, dtype=jnp.int32)
    limit = index * skip // STRIDE
    visible = (jnp.arange(blocks, dtype=jnp.int32)[None, :] <= limit[:, None])[:, None, None, :]
    scores = jnp.where(visible, scores, -1e30)
    peak = jnp.max(scores, -1, keepdims=True)
    weights = jnp.where(visible, jnp.exp(scores - peak), 0.0)
    probs = (weights / jnp.sum(weights, -1, keepdims=True)).astype(jnp.bfloat16)
    attended = jnp.einsum("qhgb,bhd->qhgd", probs, all_values, preferred_element_type=jnp.float32)
    return attended.astype(jnp.bfloat16).reshape(count, -1)


def attend_whole(queries, keys, values, key_position, compress_keys, compress_values, skip):
    rows = gather_over(keys, "seq", 0)
    vals = gather_over(values, "seq", 0)
    query = gather_over(queries, "seq", 0)
    none = jnp.zeros((STRIDE, rows.shape[1]), rows.dtype)
    comp_keys = compress_rows(rows, none, key_position, compress_keys)
    comp_values = compress_rows(vals, none, key_position, compress_values)
    heads = rows.shape[1] // HEAD_DIM
    group = query.shape[1] // HEAD_DIM // heads
    return attend(
        query.reshape(-1, heads, group, HEAD_DIM),
        comp_keys.reshape(-1, heads, HEAD_DIM),
        comp_values.reshape(-1, heads, HEAD_DIM),
        0,
        skip,
    )


def attend_segments(queries, keys, values, key_position, compress_keys, compress_values, skip):
    following = from_behind((keys[:STRIDE], values[:STRIDE]), "seq", -1)
    comp_keys = compress_rows(keys, following[0], key_position, compress_keys)
    comp_values = compress_rows(values, following[1], key_position, compress_values)
    every = lax.all_gather(jnp.stack([comp_keys, comp_values], 0), "seq", axis=1, tiled=True)
    heads = keys.shape[1] // HEAD_DIM
    group = queries.shape[1] // HEAD_DIM // heads
    blocks = every.shape[1]
    attended = attend(
        queries.reshape(-1, heads, group, HEAD_DIM),
        every[0].reshape(blocks, heads, HEAD_DIM),
        every[1].reshape(blocks, heads, HEAD_DIM),
        lax.axis_index("seq") * queries.shape[0],
        skip,
    )
    return lax.all_gather(attended, "seq", axis=0, tiled=True)


EVERY = ("seq", "mp", "batch")


def log_probs(logits, wanted, offset):
    picked = picked_logit(logits, offset, wanted)
    local_top = jnp.max(logits, 1)
    devices = lax.axis_size(EVERY)
    if devices > SPREAD:
        top = lax.pmax(local_top, EVERY)
        local_sum = jnp.sum(jnp.exp(logits - top[:, None]), 1)
        total, target_logit = lax.psum((local_sum, picked), EVERY)
        return target_logit - (top + jnp.log(total))
    local_sum = jnp.sum(jnp.exp(logits - local_top[:, None]), 1)
    mine = jnp.concatenate([local_top, local_sum, picked], 0)
    sent = jnp.broadcast_to(mine[None, :], (devices, mine.shape[0]))
    tops, sums, hits = jnp.split(lax.all_to_all(sent, EVERY, 0, 0, tiled=True), 3, 1)
    top = jnp.max(tops, 0)
    total = jnp.sum(sums * jnp.exp(tops - top[None, :]), 0)
    return jnp.sum(hits, 0) - (top + jnp.log(total))


def large_mesh(
    queries,
    keys,
    values,
    key_position,
    compress_keys,
    compress_values,
    out_proj,
    residual,
    norm_gain,
    lm_head,
    targets,
    lengths,
):
    seq_pos = lax.axis_index("seq")
    batch_pos = lax.axis_index("batch")
    qcount = queries.shape[1]
    skip = keys.shape[1] // qcount
    rollouts, scored = targets.shape
    attending = attend_whole if direct("seq") else attend_segments
    attended = attending(
        queries[0], keys[0], values[0], key_position, compress_keys, compress_values, skip
    )
    part = jnp.dot(attended, out_proj, preferred_element_type=jnp.float32)
    summed = sum_over(part, "mp")
    hidden = (residual[batch_pos].astype(jnp.float32) + summed).astype(jnp.bfloat16)
    whole = gather_over(gather_over(hidden, "batch", 0), "seq", 1)
    normed = normalize(whole, norm_gain)
    logits = vocab_logits(normed, lm_head)
    offset = lax.axis_index(EVERY) * lm_head.shape[0]
    by_rollout = log_probs(logits, targets.reshape(-1), offset).reshape(rollouts, scored)
    spots = jnp.arange(scored, dtype=jnp.int32) * skip + BLOCK - 1
    valid = (spots[None, :] < lengths[:, None]).astype(jnp.float32)
    count = jnp.sum(valid)
    token_logprob = lax.dynamic_slice(by_rollout, (batch_pos, seq_pos * qcount), (1, qcount))
    sums = jnp.sum(valid * by_rollout, 1) / count
    rollout_score = sums[batch_pos][None]
    return (token_logprob, rollout_score)


VMEM = pl.BlockSpec(memory_space=pltpu.VMEM)
SMEM = pl.BlockSpec(memory_space=pltpu.SMEM)
NT = (((1,), (1,)), ((), ()))
LANES = 128
FILL = 20_000_000_000


def swap(block):
    return lax.ppermute(block, "seq", [(0, 1), (1, 0)])


def crossed(block, axis, distance):
    count = lax.axis_size(axis)
    route = [
        (core * count + i, (1 - core) * count + (i ^ distance))
        for core in range(2)
        for i in range(count)
    ]
    return lax.ppermute(block, ("seq", axis), route)


def crossed_all(block, axis):
    return [crossed(block, axis, d) for d in range(lax.axis_size(axis) - 1, 0, -1)][::-1]


def compress_all(rows, position, weight):
    blocks = rows.shape[1] // STRIDE - 1
    total = None
    for first in range(0, BLOCK, 2):
        sides = []
        for i in (first, first + 1):
            offset = position[i : i + 1, :]
            sides.append(
                jnp.concatenate(
                    [
                        rows[head, pl.ds(i, blocks, stride=STRIDE), :] + offset
                        for head in range(rows.shape[0])
                    ],
                    0,
                )
            )
        left = jnp.concatenate(sides, 1).astype(jnp.bfloat16)
        right = weight[first * HEAD_DIM : (first + 2) * HEAD_DIM, :]
        term = jnp.dot(left, right, preferred_element_type=jnp.float32)
        total = term if total is None else total + term
    total = total.astype(jnp.bfloat16)
    return [total[h * blocks : (h + 1) * blocks, :] for h in range(rows.shape[0])]


def attention_kernel(
    k_mine,
    k_other,
    v_mine,
    v_other,
    q_mine,
    q_other,
    position,
    weight_k,
    weight_v,
    visible,
    out,
    k_rows,
    v_rows,
    q_rows,
):
    core = lax.axis_index("seq")
    length, width = k_mine.shape
    heads = width // HEAD_DIM
    for rows, mine, other in ((k_rows, k_mine, k_other), (v_rows, v_mine, v_other)):
        for place, half in ((core, mine), (1 - core, other)):
            where = pl.ds(pl.multiple_of(place * length, length), length)
            for head in range(heads):
                rows[head, where, :] = half[:, head * HEAD_DIM : (head + 1) * HEAD_DIM].astype(
                    jnp.float32
                )
        rows[:, 2 * length :, :] = jnp.zeros((heads, STRIDE, HEAD_DIM), jnp.float32)
    few = q_mine.shape[0]
    mine = q_mine[...].astype(jnp.float32)
    other = q_other[...].astype(jnp.float32)
    q_rows[:few, :] = jnp.where(core == 0, mine, other)
    q_rows[few:, :] = jnp.where(core == 0, other, mine)
    count = 2 * few
    keys = compress_all(k_rows, position, weight_k)
    values = compress_all(v_rows, position, weight_v)
    group = q_rows.shape[1] // HEAD_DIM // heads
    seen = visible[...].reshape(group * count, visible.shape[2]) > 0.0
    lanes = []
    for head in range(heads):
        query = jnp.concatenate(
            [
                q_rows[:, (head * group + g) * HEAD_DIM : (head * group + g + 1) * HEAD_DIM]
                for g in range(group)
            ],
            0,
        ).astype(jnp.bfloat16)
        scores = lax.dot_general(query, keys[head], NT, preferred_element_type=jnp.float32)
        scores = jnp.where(seen, scores * (1.0 / math.sqrt(HEAD_DIM)), -1e30)
        peak = jnp.max(scores, -1, keepdims=True)
        weights = jnp.where(seen, jnp.exp(scores - peak), 0.0)
        probs = (weights / jnp.sum(weights, -1, keepdims=True)).astype(jnp.bfloat16)
        attended = jnp.dot(probs, values[head], preferred_element_type=jnp.float32)
        attended = attended.astype(jnp.bfloat16).astype(jnp.float32)
        lanes += [attended[g * count : (g + 1) * count, :] for g in range(group)]
    out[...] = jnp.concatenate(lanes, 1).astype(jnp.bfloat16)


def product_kernel(attended, out_proj, residual, part):
    mine = residual[lax.axis_index("batch")].astype(jnp.float32)
    part[...] = jnp.where(lax.axis_index("mp") == 0, mine, 0.0) + jnp.dot(
        attended[...], out_proj[...], preferred_element_type=jnp.float32
    )


def visible_kernel(skip, visible):
    row = lax.broadcasted_iota(jnp.int32, visible.shape, 1)
    block = lax.broadcasted_iota(jnp.int32, visible.shape, 2)
    visible[...] = (block <= row * skip // STRIDE).astype(jnp.float32)


def visible_blocks(group, count, blocks, skip):
    return pl.pallas_call(
        functools.partial(visible_kernel, skip),
        out_shape=jax.ShapeDtypeStruct((group, count, blocks), jnp.float32),
        out_specs=VMEM,
        compiler_params=pltpu.CompilerParams(vmem_limit_bytes=4 << 20),
        cost_estimate=pl.CostEstimate(flops=FILL, bytes_accessed=0, transcendentals=0),
        name="visible",
    )()


def attention(keys, values, queries, key_position, compress_keys, compress_values, skip):
    length, width = keys.shape
    heads = width // HEAD_DIM
    count = 2 * queries.shape[0]
    group = queries.shape[1] // HEAD_DIM // heads
    rows = pltpu.VMEM((heads, 2 * length + STRIDE, HEAD_DIM), jnp.float32)
    return pl.pallas_call(
        attention_kernel,
        out_shape=jax.ShapeDtypeStruct((count, queries.shape[1]), jnp.bfloat16),
        in_specs=[VMEM] * 10,
        out_specs=VMEM,
        scratch_shapes=[rows, rows, pltpu.VMEM((count, queries.shape[1]), jnp.float32)],
        compiler_params=pltpu.CompilerParams(vmem_limit_bytes=16 << 20),
        cost_estimate=pl.CostEstimate(
            flops=16 * length * width * HEAD_DIM,
            bytes_accessed=2 * (compress_keys.size + compress_values.size),
            transcendentals=count * 1024,
        ),
        name="attention",
    )(
        keys,
        swap(keys),
        values,
        swap(values),
        queries,
        swap(queries),
        key_position,
        compress_keys,
        compress_values,
        visible_blocks(group, count, 2 * length // STRIDE, skip),
    )


def product(attended, out_proj, residual):
    return pl.pallas_call(
        product_kernel,
        out_shape=jax.ShapeDtypeStruct(residual.shape[1:], jnp.float32),
        in_specs=[VMEM] * 3,
        out_specs=VMEM,
        compiler_params=pltpu.CompilerParams(vmem_limit_bytes=16 << 20),
        cost_estimate=pl.CostEstimate(
            flops=2 * attended.shape[0] * out_proj.size,
            bytes_accessed=2 * out_proj.size,
            transcendentals=0,
        ),
        name="product",
    )(attended, out_proj, residual)


def logits_kernel(batch, scored, skip, *refs):
    near, far = refs[:batch], refs[batch : 2 * batch]
    gain, lm_head, facts, sent = refs[2 * batch :]
    core = lax.axis_index("seq")
    blocks = []
    for n, f in zip(near, far):
        n = n[...].astype(jnp.float32)
        f = f[...].astype(jnp.float32)
        blocks.append(
            jnp.concatenate([jnp.where(core == 0, n, f), jnp.where(core == 0, f, n)], 1)
        )
    hidden = jnp.concatenate(by_position(blocks, "batch"), 0)
    meansq = jnp.mean(hidden * hidden, -1, keepdims=True)
    normed = (hidden * lax.rsqrt(meansq + 1e-05) * gain[...]).astype(jnp.bfloat16)
    logits = lax.dot_general(lm_head[...], normed, NT, preferred_element_type=jnp.float32)
    share, rows = logits.shape
    offset = device_index() * share
    ids = offset + lax.broadcasted_iota(jnp.int32, (share, rows), 0)
    top = jnp.max(logits, 0, keepdims=True)
    total = jnp.sum(jnp.exp(logits - top), 0, keepdims=True)
    picked = jnp.sum(jnp.where(ids == facts[0:1, :], logits, 0.0), 0, keepdims=True)
    spots = lax.broadcasted_iota(jnp.int32, (1, rows), 1) % scored * skip + BLOCK - 1
    valid = (spots < facts[1:2, :]).astype(jnp.float32)
    known = [top, total, picked, valid]
    if sent.shape[1] > 4 * rows:
        known.append(jnp.zeros((1, sent.shape[1] - 4 * rows), jnp.float32))
    sent[...] = jnp.broadcast_to(jnp.concatenate(known, 1), sent.shape)


def device_index():
    index = 0
    for axis in EVERY:
        index = index * lax.axis_size(axis) + lax.axis_index(axis)
    return index


def share_statistics(near, far, norm_gain, lm_head, targets, lengths, skip):
    scored = targets.shape[1]
    facts = jnp.stack([targets.reshape(-1), jnp.repeat(lengths, scored)], 0)
    rows = facts.shape[1]
    across = -(-4 * rows // LANES) * LANES
    return pl.pallas_call(
        functools.partial(logits_kernel, len(near), scored, skip),
        out_shape=jax.ShapeDtypeStruct((lax.axis_size(EVERY), across), jnp.float32),
        in_specs=[VMEM] * (2 * len(near) + 3),
        out_specs=VMEM,
        compiler_params=pltpu.CompilerParams(vmem_limit_bytes=16 << 20),
        cost_estimate=pl.CostEstimate(
            flops=2 * rows * lm_head.size, bytes_accessed=2 * lm_head.size, transcendentals=rows * 1024
        ),
        name="statistics",
    )(*near, *far, norm_gain.reshape(1, -1), lm_head, facts)


def score_kernel(rows, scored, few, got, token, score):
    tops = got[:, :rows]
    top = jnp.max(tops, 0, keepdims=True)
    total = jnp.sum(got[:, rows : 2 * rows] * jnp.exp(tops - top), 0, keepdims=True)
    picked = jnp.sum(got[:, 2 * rows : 3 * rows], 0, keepdims=True)
    logprob = picked - (top + jnp.log(total))
    index = lax.broadcasted_iota(jnp.int32, (1, rows), 1)
    valid = got[0:1, 3 * rows : 4 * rows]
    count = jnp.sum(valid, 1, keepdims=True)
    batch = lax.axis_index("batch")
    mine = jnp.where(index // scored == batch, valid * logprob, 0.0)
    score[...] = jnp.sum(mine, 1, keepdims=True) / count
    start = batch * scored + lax.axis_index("seq") * few
    out = jnp.zeros((1, few), jnp.float32)
    lane = lax.broadcasted_iota(jnp.int32, (1, few), 1)
    for j in range(few):
        value = jnp.sum(jnp.where(index == start + j, logprob, 0.0), 1, keepdims=True)
        out = jnp.where(lane == j, value, out)
    token[...] = out


def final_scores(got, rows, scored, few):
    token, score = pl.pallas_call(
        functools.partial(score_kernel, rows, scored, few),
        out_shape=(
            jax.ShapeDtypeStruct((1, few), jnp.float32),
            jax.ShapeDtypeStruct((1, 1), jnp.float32),
        ),
        in_specs=[VMEM],
        out_specs=(VMEM, VMEM),
        compiler_params=pltpu.CompilerParams(vmem_limit_bytes=4 << 20),
        name="scores",
    )(got)
    return token, score.reshape(1)


def small_mesh(
    queries,
    keys,
    values,
    key_position,
    compress_keys,
    compress_values,
    out_proj,
    residual,
    norm_gain,
    lm_head,
    targets,
    lengths,
):
    few = queries.shape[1]
    skip = keys.shape[1] // few
    attended = attention(
        keys[0], values[0], queries[0], key_position, compress_keys, compress_values, skip
    )
    part = product(attended, out_proj, residual)
    parts = [swap(part)] + crossed_all(part, "mp")
    far = [pair_sum(parts).astype(jnp.bfloat16)]
    near = crossed_all(far[0], "batch")
    far += [swap(block) for block in near]
    near = [swap(far[0])] + near
    sent = share_statistics(near, far, norm_gain, lm_head, targets, lengths, skip)
    got = lax.all_to_all(sent, EVERY, 0, 0, tiled=True)
    return final_scores(got, targets.size, targets.shape[1], few)


def body(*arrays):
    small = (
        lax.axis_size("seq") == 2
        and direct("mp")
        and direct("batch")
        and lax.axis_size(EVERY) <= SPREAD
    )
    return small_mesh(*arrays) if small else large_mesh(*arrays)


def solution(mesh):
    in_specs = (
        P("batch", "seq", "mp"),
        P("batch", "seq", "mp"),
        P("batch", "seq", "mp"),
        P(),
        P(),
        P(),
        P("mp", "seq"),
        P(None, None, "seq"),
        P(),
        P(("seq", "mp", "batch"), None),
        P(),
        P(),
    )
    out_specs = (P("batch", "seq"), P("batch"))
    return jax.shard_map(body, mesh=mesh, in_specs=in_specs, out_specs=out_specs, check_vma=False)
```

```python
import functools
import math

import jax
import jax.numpy as jnp
from jax import lax
from jax.experimental import pallas as pl
from jax.experimental.pallas import tpu as pltpu
from jax.sharding import PartitionSpec as P


HEAD_DIM = 128
BLOCK = 32
STRIDE = 16


def from_behind(block, axis, distance):
    devices = range(lax.axis_size(axis))
    route = [(i - distance, i) for i in devices if i - distance in devices]
    return lax.ppermute(block, axis, route)


def compress_rows(rows, following, position, weight):
    extended = jnp.concatenate([rows, following], 0)
    count = rows.shape[0] // STRIDE
    heads = rows.shape[1] // HEAD_DIM
    shaped = extended.reshape(count + 1, STRIDE, heads, HEAD_DIM)
    blocks = jnp.concatenate([shaped[:-1], shaped[1:]], 1)
    blocks = (blocks.astype(jnp.float32) + position[None, :, None, :]).astype(jnp.bfloat16)
    mapped = jnp.einsum(
        "bjhd,jde->bhe",
        blocks,
        weight.reshape(BLOCK, HEAD_DIM, HEAD_DIM),
        preferred_element_type=jnp.float32,
    )
    return mapped.astype(jnp.bfloat16).reshape(count, heads * HEAD_DIM)


def normalize(hidden, gain):
    widened = hidden.astype(jnp.float32)
    meansq = jnp.mean(widened * widened, -1, keepdims=True)
    return (widened * lax.rsqrt(meansq + 1e-05) * gain).astype(jnp.bfloat16)


def vocab_logits(normed, rows):
    return lax.dot_general(
        normed, rows, (((1,), (1,)), ((), ())), preferred_element_type=jnp.float32
    )


def picked_logit(logits, offset, wanted):
    columns = offset + jnp.arange(logits.shape[1], dtype=jnp.int32)
    hits = columns[None, :] == wanted[:, None]
    return jnp.sum(jnp.where(hits, logits, 0.0), 1)


DIRECT = 4
SPREAD = 64


def pairs(axis, distance):
    return [(i, i ^ distance) for i in range(lax.axis_size(axis))]


def direct(axis):
    count = lax.axis_size(axis)
    return count <= DIRECT and count & (count - 1) == 0


def exchange(block, axis):
    return [block] + [
        lax.ppermute(block, axis, pairs(axis, distance))
        for distance in range(1, lax.axis_size(axis))
    ]


def by_position(blocks, axis):
    place = lax.axis_index(axis)
    step = 1
    while step < len(blocks):
        odd = (place // step) % 2 == 1
        blocks = [jnp.where(odd, blocks[i ^ step], blocks[i]) for i in range(len(blocks))]
        step *= 2
    return blocks


def pair_sum(blocks):
    while len(blocks) > 1:
        blocks = [blocks[i] + blocks[i + 1] for i in range(0, len(blocks), 2)]
    return blocks[0]


def sum_over(part, axis):
    if direct(axis):
        return pair_sum(exchange(part, axis))
    return lax.psum(part, axis)


def gather_over(block, axis, dimension):
    if direct(axis):
        return jnp.concatenate(by_position(exchange(block, axis), axis), dimension)
    return lax.all_gather(block, axis, axis=dimension, tiled=True)


def attend(query, all_keys, all_values, first, skip):
    count = query.shape[0]
    blocks = all_keys.shape[0]
    scores = jnp.einsum("qhgd,bhd->qhgb", query, all_keys, preferred_element_type=jnp.float32) * (
        1.0 / math.sqrt(HEAD_DIM)
    )
    index = first + jnp.arange(count, dtype=jnp.int32)
    limit = index * skip // STRIDE
    visible = (jnp.arange(blocks, dtype=jnp.int32)[None, :] <= limit[:, None])[:, None, None, :]
    scores = jnp.where(visible, scores, -1e30)
    peak = jnp.max(scores, -1, keepdims=True)
    weights = jnp.where(visible, jnp.exp(scores - peak), 0.0)
    probs = (weights / jnp.sum(weights, -1, keepdims=True)).astype(jnp.bfloat16)
    attended = jnp.einsum("qhgb,bhd->qhgd", probs, all_values, preferred_element_type=jnp.float32)
    return attended.astype(jnp.bfloat16).reshape(count, -1)


def attend_whole(queries, keys, values, key_position, compress_keys, compress_values, skip):
    rows = gather_over(keys, "seq", 0)
    vals = gather_over(values, "seq", 0)
    query = gather_over(queries, "seq", 0)
    none = jnp.zeros((STRIDE, rows.shape[1]), rows.dtype)
    comp_keys = compress_rows(rows, none, key_position, compress_keys)
    comp_values = compress_rows(vals, none, key_position, compress_values)
    heads = rows.shape[1] // HEAD_DIM
    group = query.shape[1] // HEAD_DIM // heads
    return attend(
        query.reshape(-1, heads, group, HEAD_DIM),
        comp_keys.reshape(-1, heads, HEAD_DIM),
        comp_values.reshape(-1, heads, HEAD_DIM),
        0,
        skip,
    )


def attend_segments(queries, keys, values, key_position, compress_keys, compress_values, skip):
    following = from_behind((keys[:STRIDE], values[:STRIDE]), "seq", -1)
    comp_keys = compress_rows(keys, following[0], key_position, compress_keys)
    comp_values = compress_rows(values, following[1], key_position, compress_values)
    every = lax.all_gather(jnp.stack([comp_keys, comp_values], 0), "seq", axis=1, tiled=True)
    heads = keys.shape[1] // HEAD_DIM
    group = queries.shape[1] // HEAD_DIM // heads
    blocks = every.shape[1]
    attended = attend(
        queries.reshape(-1, heads, group, HEAD_DIM),
        every[0].reshape(blocks, heads, HEAD_DIM),
        every[1].reshape(blocks, heads, HEAD_DIM),
        lax.axis_index("seq") * queries.shape[0],
        skip,
    )
    return lax.all_gather(attended, "seq", axis=0, tiled=True)


EVERY = ("seq", "mp", "batch")


def log_probs(logits, wanted, offset):
    picked = picked_logit(logits, offset, wanted)
    local_top = jnp.max(logits, 1)
    devices = lax.axis_size(EVERY)
    if devices > SPREAD:
        top = lax.pmax(local_top, EVERY)
        local_sum = jnp.sum(jnp.exp(logits - top[:, None]), 1)
        total, target_logit = lax.psum((local_sum, picked), EVERY)
        return target_logit - (top + jnp.log(total))
    local_sum = jnp.sum(jnp.exp(logits - local_top[:, None]), 1)
    mine = jnp.concatenate([local_top, local_sum, picked], 0)
    sent = jnp.broadcast_to(mine[None, :], (devices, mine.shape[0]))
    tops, sums, hits = jnp.split(lax.all_to_all(sent, EVERY, 0, 0, tiled=True), 3, 1)
    top = jnp.max(tops, 0)
    total = jnp.sum(sums * jnp.exp(tops - top[None, :]), 0)
    return jnp.sum(hits, 0) - (top + jnp.log(total))


def large_mesh(
    queries,
    keys,
    values,
    key_position,
    compress_keys,
    compress_values,
    out_proj,
    residual,
    norm_gain,
    lm_head,
    targets,
    lengths,
):
    seq_pos = lax.axis_index("seq")
    batch_pos = lax.axis_index("batch")
    qcount = queries.shape[1]
    skip = keys.shape[1] // qcount
    rollouts, scored = targets.shape
    attending = attend_whole if direct("seq") else attend_segments
    attended = attending(
        queries[0], keys[0], values[0], key_position, compress_keys, compress_values, skip
    )
    part = jnp.dot(attended, out_proj, preferred_element_type=jnp.float32)
    summed = sum_over(part, "mp")
    hidden = (residual[batch_pos].astype(jnp.float32) + summed).astype(jnp.bfloat16)
    whole = gather_over(gather_over(hidden, "batch", 0), "seq", 1)
    normed = normalize(whole, norm_gain)
    logits = vocab_logits(normed, lm_head)
    offset = lax.axis_index(EVERY) * lm_head.shape[0]
    by_rollout = log_probs(logits, targets.reshape(-1), offset).reshape(rollouts, scored)
    spots = jnp.arange(scored, dtype=jnp.int32) * skip + BLOCK - 1
    valid = (spots[None, :] < lengths[:, None]).astype(jnp.float32)
    count = jnp.sum(valid)
    token_logprob = lax.dynamic_slice(by_rollout, (batch_pos, seq_pos * qcount), (1, qcount))
    sums = jnp.sum(valid * by_rollout, 1) / count
    rollout_score = sums[batch_pos][None]
    return (token_logprob, rollout_score)


VMEM = pl.BlockSpec(memory_space=pltpu.VMEM)
SMEM = pl.BlockSpec(memory_space=pltpu.SMEM)
NT = (((1,), (1,)), ((), ()))
LANES = 128
FILL = 20_000_000_000


def swap(block):
    return lax.ppermute(block, "seq", [(0, 1), (1, 0)])


def crossed(block, axis, distance):
    count = lax.axis_size(axis)
    route = [
        (core * count + i, (1 - core) * count + (i ^ distance))
        for core in range(2)
        for i in range(count)
    ]
    return lax.ppermute(block, ("seq", axis), route)


def crossed_all(block, axis):
    return [crossed(block, axis, d) for d in range(lax.axis_size(axis) - 1, 0, -1)][::-1]


def compress_all(rows, position, weight):
    blocks = rows.shape[1] // STRIDE - 1
    total = None
    for first in range(0, BLOCK, 2):
        sides = []
        for i in (first, first + 1):
            offset = position[i : i + 1, :]
            sides.append(
                jnp.concatenate(
                    [
                        rows[head, pl.ds(i, blocks, stride=STRIDE), :] + offset
                        for head in range(rows.shape[0])
                    ],
                    0,
                )
            )
        left = jnp.concatenate(sides, 1).astype(jnp.bfloat16)
        right = weight[first * HEAD_DIM : (first + 2) * HEAD_DIM, :]
        term = jnp.dot(left, right, preferred_element_type=jnp.float32)
        total = term if total is None else total + term
    total = total.astype(jnp.bfloat16)
    return [total[h * blocks : (h + 1) * blocks, :] for h in range(rows.shape[0])]


def attention_kernel(
    k_mine,
    k_other,
    v_mine,
    v_other,
    q_mine,
    q_other,
    position,
    weight_k,
    weight_v,
    visible,
    out,
    k_rows,
    v_rows,
    q_rows,
):
    core = lax.axis_index("seq")
    length, width = k_mine.shape
    heads = width // HEAD_DIM
    for rows, mine, other in ((k_rows, k_mine, k_other), (v_rows, v_mine, v_other)):
        for place, half in ((core, mine), (1 - core, other)):
            where = pl.ds(pl.multiple_of(place * length, length), length)
            for head in range(heads):
                rows[head, where, :] = half[:, head * HEAD_DIM : (head + 1) * HEAD_DIM].astype(
                    jnp.float32
                )
        rows[:, 2 * length :, :] = jnp.zeros((heads, STRIDE, HEAD_DIM), jnp.float32)
    few = q_mine.shape[0]
    mine = q_mine[...].astype(jnp.float32)
    other = q_other[...].astype(jnp.float32)
    q_rows[:few, :] = jnp.where(core == 0, mine, other)
    q_rows[few:, :] = jnp.where(core == 0, other, mine)
    count = 2 * few
    keys = compress_all(k_rows, position, weight_k)
    values = compress_all(v_rows, position, weight_v)
    group = q_rows.shape[1] // HEAD_DIM // heads
    seen = visible[...].reshape(group * count, visible.shape[2]) > 0.0
    lanes = []
    for head in range(heads):
        query = jnp.concatenate(
            [
                q_rows[:, (head * group + g) * HEAD_DIM : (head * group + g + 1) * HEAD_DIM]
                for g in range(group)
            ],
            0,
        ).astype(jnp.bfloat16)
        scores = lax.dot_general(query, keys[head], NT, preferred_element_type=jnp.float32)
        scores = jnp.where(seen, scores * (1.0 / math.sqrt(HEAD_DIM)), -1e30)
        peak = jnp.max(scores, -1, keepdims=True)
        weights = jnp.where(seen, jnp.exp(scores - peak), 0.0)
        probs = (weights / jnp.sum(weights, -1, keepdims=True)).astype(jnp.bfloat16)
        attended = jnp.dot(probs, values[head], preferred_element_type=jnp.float32)
        attended = attended.astype(jnp.bfloat16).astype(jnp.float32)
        lanes += [attended[g * count : (g + 1) * count, :] for g in range(group)]
    out[...] = jnp.concatenate(lanes, 1).astype(jnp.bfloat16)


def product_kernel(attended, out_proj, residual, part):
    mine = residual[lax.axis_index("batch")].astype(jnp.float32)
    part[...] = jnp.where(lax.axis_index("mp") == 0, mine, 0.0) + jnp.dot(
        attended[...], out_proj[...], preferred_element_type=jnp.float32
    )


def visible_kernel(skip, visible):
    row = lax.broadcasted_iota(jnp.int32, visible.shape, 1)
    block = lax.broadcasted_iota(jnp.int32, visible.shape, 2)
    visible[...] = (block <= row * skip // STRIDE).astype(jnp.float32)


def visible_blocks(group, count, blocks, skip):
    return pl.pallas_call(
        functools.partial(visible_kernel, skip),
        out_shape=jax.ShapeDtypeStruct((group, count, blocks), jnp.float32),
        out_specs=VMEM,
        compiler_params=pltpu.CompilerParams(vmem_limit_bytes=4 << 20),
        cost_estimate=pl.CostEstimate(flops=FILL, bytes_accessed=0, transcendentals=0),
        name="visible",
    )()


def attention(keys, values, queries, key_position, compress_keys, compress_values, skip):
    length, width = keys.shape
    heads = width // HEAD_DIM
    count = 2 * queries.shape[0]
    group = queries.shape[1] // HEAD_DIM // heads
    rows = pltpu.VMEM((heads, 2 * length + STRIDE, HEAD_DIM), jnp.float32)
    return pl.pallas_call(
        attention_kernel,
        out_shape=jax.ShapeDtypeStruct((count, queries.shape[1]), jnp.bfloat16),
        in_specs=[VMEM] * 10,
        out_specs=VMEM,
        scratch_shapes=[rows, rows, pltpu.VMEM((count, queries.shape[1]), jnp.float32)],
        compiler_params=pltpu.CompilerParams(vmem_limit_bytes=16 << 20),
        cost_estimate=pl.CostEstimate(
            flops=16 * length * width * HEAD_DIM,
            bytes_accessed=2 * (compress_keys.size + compress_values.size),
            transcendentals=count * 1024,
        ),
        name="attention",
    )(
        keys,
        swap(keys),
        values,
        swap(values),
        queries,
        swap(queries),
        key_position,
        compress_keys,
        compress_values,
        visible_blocks(group, count, 2 * length // STRIDE, skip),
    )


def product(attended, out_proj, residual):
    return pl.pallas_call(
        product_kernel,
        out_shape=jax.ShapeDtypeStruct(residual.shape[1:], jnp.float32),
        in_specs=[VMEM] * 3,
        out_specs=VMEM,
        compiler_params=pltpu.CompilerParams(vmem_limit_bytes=16 << 20),
        cost_estimate=pl.CostEstimate(
            flops=2 * attended.shape[0] * out_proj.size,
            bytes_accessed=2 * out_proj.size,
            transcendentals=0,
        ),
        name="product",
    )(attended, out_proj, residual)


def logits_kernel(scored, skip, *refs):
    near_mine, near_others, far_mine, far_others, gain, lm_head, facts, sent = refs
    core = lax.axis_index("seq")
    blocks = []
    for n, f in ((near_mine, far_mine), (near_others, far_others)):
        n = n[...].astype(jnp.float32)
        f = f[...].astype(jnp.float32)
        both = jnp.concatenate([jnp.where(core == 0, n, f), jnp.where(core == 0, f, n)], 1)
        blocks += [both[r : r + scored] for r in range(0, both.shape[0], scored)]
    hidden = jnp.concatenate(by_position(blocks, "batch"), 0)
    meansq = jnp.mean(hidden * hidden, -1, keepdims=True)
    normed = (hidden * lax.rsqrt(meansq + 1e-05) * gain[...]).astype(jnp.bfloat16)
    logits = lax.dot_general(lm_head[...], normed, NT, preferred_element_type=jnp.float32)
    share, rows = logits.shape
    offset = device_index() * share
    ids = offset + lax.broadcasted_iota(jnp.int32, (share, rows), 0)
    top = jnp.max(logits, 0, keepdims=True)
    total = jnp.sum(jnp.exp(logits - top), 0, keepdims=True)
    picked = jnp.sum(jnp.where(ids == facts[0:1, :], logits, 0.0), 0, keepdims=True)
    spots = lax.broadcasted_iota(jnp.int32, (1, rows), 1) % scored * skip + BLOCK - 1
    valid = (spots < facts[1:2, :]).astype(jnp.float32)
    known = [top, total, picked, valid]
    if sent.shape[1] > 4 * rows:
        known.append(jnp.zeros((1, sent.shape[1] - 4 * rows), jnp.float32))
    sent[...] = jnp.broadcast_to(jnp.concatenate(known, 1), sent.shape)


def device_index():
    index = 0
    for axis in EVERY:
        index = index * lax.axis_size(axis) + lax.axis_index(axis)
    return index


def share_statistics(near, far, norm_gain, lm_head, targets, lengths, skip):
    scored = targets.shape[1]
    facts = jnp.stack([targets.reshape(-1), jnp.repeat(lengths, scored)], 0)
    rows = facts.shape[1]
    across = -(-4 * rows // LANES) * LANES
    return pl.pallas_call(
        functools.partial(logits_kernel, scored, skip),
        out_shape=jax.ShapeDtypeStruct((lax.axis_size(EVERY), across), jnp.float32),
        in_specs=[VMEM] * (2 * len(near) + 3),
        out_specs=VMEM,
        compiler_params=pltpu.CompilerParams(vmem_limit_bytes=16 << 20),
        cost_estimate=pl.CostEstimate(
            flops=2 * rows * lm_head.size, bytes_accessed=2 * lm_head.size, transcendentals=rows * 1024
        ),
        name="statistics",
    )(*near, *far, norm_gain.reshape(1, -1), lm_head, facts)


def score_kernel(rows, scored, few, got, token, score):
    tops = got[:, :rows]
    top = jnp.max(tops, 0, keepdims=True)
    total = jnp.sum(got[:, rows : 2 * rows] * jnp.exp(tops - top), 0, keepdims=True)
    picked = jnp.sum(got[:, 2 * rows : 3 * rows], 0, keepdims=True)
    logprob = picked - (top + jnp.log(total))
    index = lax.broadcasted_iota(jnp.int32, (1, rows), 1)
    valid = got[0:1, 3 * rows : 4 * rows]
    count = jnp.sum(valid, 1, keepdims=True)
    batch = lax.axis_index("batch")
    mine = jnp.where(index // scored == batch, valid * logprob, 0.0)
    score[...] = jnp.sum(mine, 1, keepdims=True) / count
    start = batch * scored + lax.axis_index("seq") * few
    spare = jnp.zeros((1, got.shape[1] - rows), jnp.float32)
    turned = pltpu.roll(jnp.concatenate([logprob, spare], 1), got.shape[1] - start, 1)
    token[...] = turned[:, :few]


def final_scores(got, rows, scored, few):
    token, score = pl.pallas_call(
        functools.partial(score_kernel, rows, scored, few),
        out_shape=(
            jax.ShapeDtypeStruct((1, few), jnp.float32),
            jax.ShapeDtypeStruct((1, 1), jnp.float32),
        ),
        in_specs=[VMEM],
        out_specs=(VMEM, VMEM),
        compiler_params=pltpu.CompilerParams(vmem_limit_bytes=4 << 20),
        name="scores",
    )(got)
    return token, score.reshape(1)


def small_mesh(
    queries,
    keys,
    values,
    key_position,
    compress_keys,
    compress_values,
    out_proj,
    residual,
    norm_gain,
    lm_head,
    targets,
    lengths,
):
    few = queries.shape[1]
    skip = keys.shape[1] // few
    attended = attention(
        keys[0], values[0], queries[0], key_position, compress_keys, compress_values, skip
    )
    part = product(attended, out_proj, residual)
    parts = [swap(part)]
    parts += crossed_all(part, "mp")
    far = [pair_sum(parts).astype(jnp.bfloat16)]
    near = crossed_all(far[0], "batch")
    near = [swap(far[0]), jnp.concatenate(near, 0)]
    far.append(swap(near[1]))
    sent = share_statistics(near, far, norm_gain, lm_head, targets, lengths, skip)
    got = lax.all_to_all(sent, EVERY, 0, 0, tiled=True)
    return final_scores(got, targets.size, targets.shape[1], few)


def body(*arrays):
    small = (
        lax.axis_size("seq") == 2
        and direct("mp")
        and direct("batch")
        and lax.axis_size(EVERY) <= SPREAD
    )
    return small_mesh(*arrays) if small else large_mesh(*arrays)


def solution(mesh):
    in_specs = (
        P("batch", "seq", "mp"),
        P("batch", "seq", "mp"),
        P("batch", "seq", "mp"),
        P(),
        P(),
        P(),
        P("mp", "seq"),
        P(None, None, "seq"),
        P(),
        P(("seq", "mp", "batch"), None),
        P(),
        P(),
    )
    out_specs = (P("batch", "seq"), P("batch"))
    return jax.shard_map(body, mesh=mesh, in_specs=in_specs, out_specs=out_specs, check_vma=False)
```

```python
import functools
import math

import jax
import jax.numpy as jnp
from jax import lax
from jax.experimental import pallas as pl
from jax.experimental.pallas import tpu as pltpu
from jax.sharding import PartitionSpec as P


HEAD_DIM = 128
BLOCK = 32
STRIDE = 16


def from_behind(block, axis, distance):
    devices = range(lax.axis_size(axis))
    route = [(i - distance, i) for i in devices if i - distance in devices]
    return lax.ppermute(block, axis, route)


def compress_rows(rows, following, position, weight):
    extended = jnp.concatenate([rows, following], 0)
    count = rows.shape[0] // STRIDE
    heads = rows.shape[1] // HEAD_DIM
    shaped = extended.reshape(count + 1, STRIDE, heads, HEAD_DIM)
    blocks = jnp.concatenate([shaped[:-1], shaped[1:]], 1)
    blocks = (blocks.astype(jnp.float32) + position[None, :, None, :]).astype(jnp.bfloat16)
    mapped = jnp.einsum(
        "bjhd,jde->bhe",
        blocks,
        weight.reshape(BLOCK, HEAD_DIM, HEAD_DIM),
        preferred_element_type=jnp.float32,
    )
    return mapped.astype(jnp.bfloat16).reshape(count, heads * HEAD_DIM)


def normalize(hidden, gain):
    widened = hidden.astype(jnp.float32)
    meansq = jnp.mean(widened * widened, -1, keepdims=True)
    return (widened * lax.rsqrt(meansq + 1e-05) * gain).astype(jnp.bfloat16)


def vocab_logits(normed, rows):
    return lax.dot_general(
        normed, rows, (((1,), (1,)), ((), ())), preferred_element_type=jnp.float32
    )


def picked_logit(logits, offset, wanted):
    columns = offset + jnp.arange(logits.shape[1], dtype=jnp.int32)
    hits = columns[None, :] == wanted[:, None]
    return jnp.sum(jnp.where(hits, logits, 0.0), 1)


DIRECT = 4
SPREAD = 64


def pairs(axis, distance):
    return [(i, i ^ distance) for i in range(lax.axis_size(axis))]


def direct(axis):
    count = lax.axis_size(axis)
    return count <= DIRECT and count & (count - 1) == 0


def exchange(block, axis):
    return [block] + [
        lax.ppermute(block, axis, pairs(axis, distance))
        for distance in range(1, lax.axis_size(axis))
    ]


def by_position(blocks, axis):
    place = lax.axis_index(axis)
    step = 1
    while step < len(blocks):
        odd = (place // step) % 2 == 1
        blocks = [jnp.where(odd, blocks[i ^ step], blocks[i]) for i in range(len(blocks))]
        step *= 2
    return blocks


def pair_sum(blocks):
    while len(blocks) > 1:
        blocks = [blocks[i] + blocks[i + 1] for i in range(0, len(blocks), 2)]
    return blocks[0]


def sum_over(part, axis):
    if direct(axis):
        return pair_sum(exchange(part, axis))
    return lax.psum(part, axis)


def gather_over(block, axis, dimension):
    if direct(axis):
        return jnp.concatenate(by_position(exchange(block, axis), axis), dimension)
    return lax.all_gather(block, axis, axis=dimension, tiled=True)


def attend(query, all_keys, all_values, first, skip):
    count = query.shape[0]
    blocks = all_keys.shape[0]
    scores = jnp.einsum("qhgd,bhd->qhgb", query, all_keys, preferred_element_type=jnp.float32) * (
        1.0 / math.sqrt(HEAD_DIM)
    )
    index = first + jnp.arange(count, dtype=jnp.int32)
    limit = index * skip // STRIDE
    visible = (jnp.arange(blocks, dtype=jnp.int32)[None, :] <= limit[:, None])[:, None, None, :]
    scores = jnp.where(visible, scores, -1e30)
    peak = jnp.max(scores, -1, keepdims=True)
    weights = jnp.where(visible, jnp.exp(scores - peak), 0.0)
    probs = (weights / jnp.sum(weights, -1, keepdims=True)).astype(jnp.bfloat16)
    attended = jnp.einsum("qhgb,bhd->qhgd", probs, all_values, preferred_element_type=jnp.float32)
    return attended.astype(jnp.bfloat16).reshape(count, -1)


def attend_whole(queries, keys, values, key_position, compress_keys, compress_values, skip):
    rows = gather_over(keys, "seq", 0)
    vals = gather_over(values, "seq", 0)
    query = gather_over(queries, "seq", 0)
    none = jnp.zeros((STRIDE, rows.shape[1]), rows.dtype)
    comp_keys = compress_rows(rows, none, key_position, compress_keys)
    comp_values = compress_rows(vals, none, key_position, compress_values)
    heads = rows.shape[1] // HEAD_DIM
    group = query.shape[1] // HEAD_DIM // heads
    return attend(
        query.reshape(-1, heads, group, HEAD_DIM),
        comp_keys.reshape(-1, heads, HEAD_DIM),
        comp_values.reshape(-1, heads, HEAD_DIM),
        0,
        skip,
    )


def attend_segments(queries, keys, values, key_position, compress_keys, compress_values, skip):
    following = from_behind((keys[:STRIDE], values[:STRIDE]), "seq", -1)
    comp_keys = compress_rows(keys, following[0], key_position, compress_keys)
    comp_values = compress_rows(values, following[1], key_position, compress_values)
    every = lax.all_gather(jnp.stack([comp_keys, comp_values], 0), "seq", axis=1, tiled=True)
    heads = keys.shape[1] // HEAD_DIM
    group = queries.shape[1] // HEAD_DIM // heads
    blocks = every.shape[1]
    attended = attend(
        queries.reshape(-1, heads, group, HEAD_DIM),
        every[0].reshape(blocks, heads, HEAD_DIM),
        every[1].reshape(blocks, heads, HEAD_DIM),
        lax.axis_index("seq") * queries.shape[0],
        skip,
    )
    return lax.all_gather(attended, "seq", axis=0, tiled=True)


EVERY = ("seq", "mp", "batch")


def log_probs(logits, wanted, offset):
    picked = picked_logit(logits, offset, wanted)
    local_top = jnp.max(logits, 1)
    devices = lax.axis_size(EVERY)
    if devices > SPREAD:
        top = lax.pmax(local_top, EVERY)
        local_sum = jnp.sum(jnp.exp(logits - top[:, None]), 1)
        total, target_logit = lax.psum((local_sum, picked), EVERY)
        return target_logit - (top + jnp.log(total))
    local_sum = jnp.sum(jnp.exp(logits - local_top[:, None]), 1)
    mine = jnp.concatenate([local_top, local_sum, picked], 0)
    sent = jnp.broadcast_to(mine[None, :], (devices, mine.shape[0]))
    tops, sums, hits = jnp.split(lax.all_to_all(sent, EVERY, 0, 0, tiled=True), 3, 1)
    top = jnp.max(tops, 0)
    total = jnp.sum(sums * jnp.exp(tops - top[None, :]), 0)
    return jnp.sum(hits, 0) - (top + jnp.log(total))


def large_mesh(
    queries,
    keys,
    values,
    key_position,
    compress_keys,
    compress_values,
    out_proj,
    residual,
    norm_gain,
    lm_head,
    targets,
    lengths,
):
    seq_pos = lax.axis_index("seq")
    batch_pos = lax.axis_index("batch")
    qcount = queries.shape[1]
    skip = keys.shape[1] // qcount
    rollouts, scored = targets.shape
    attending = attend_whole if direct("seq") else attend_segments
    attended = attending(
        queries[0], keys[0], values[0], key_position, compress_keys, compress_values, skip
    )
    part = jnp.dot(attended, out_proj, preferred_element_type=jnp.float32)
    summed = sum_over(part, "mp")
    hidden = (residual[batch_pos].astype(jnp.float32) + summed).astype(jnp.bfloat16)
    whole = gather_over(gather_over(hidden, "batch", 0), "seq", 1)
    normed = normalize(whole, norm_gain)
    logits = vocab_logits(normed, lm_head)
    offset = lax.axis_index(EVERY) * lm_head.shape[0]
    by_rollout = log_probs(logits, targets.reshape(-1), offset).reshape(rollouts, scored)
    spots = jnp.arange(scored, dtype=jnp.int32) * skip + BLOCK - 1
    valid = (spots[None, :] < lengths[:, None]).astype(jnp.float32)
    count = jnp.sum(valid)
    token_logprob = lax.dynamic_slice(by_rollout, (batch_pos, seq_pos * qcount), (1, qcount))
    sums = jnp.sum(valid * by_rollout, 1) / count
    rollout_score = sums[batch_pos][None]
    return (token_logprob, rollout_score)


VMEM = pl.BlockSpec(memory_space=pltpu.VMEM)
SMEM = pl.BlockSpec(memory_space=pltpu.SMEM)
NT = (((1,), (1,)), ((), ()))
LANES = 128
SUBLANES = 8
FILL = 20_000_000_000


def swap(block):
    return lax.ppermute(block, "seq", [(0, 1), (1, 0)])


def crossed(block, axis, distance):
    count = lax.axis_size(axis)
    route = [
        (core * count + i, (1 - core) * count + (i ^ distance))
        for core in range(2)
        for i in range(count)
    ]
    return lax.ppermute(block, ("seq", axis), route)


def crossed_all(block, axis):
    return [crossed(block, axis, d) for d in range(lax.axis_size(axis) - 1, 0, -1)][::-1]


def compress_all(rows, position, weight):
    heads, _, blocks, _ = rows.shape
    halves = []
    for half in range(BLOCK // STRIDE):
        columns = []
        for i in range(STRIDE):
            offset = position[half * STRIDE + i : half * STRIDE + i + 1, :]
            block = [rows[head, i] + offset for head in range(heads)]
            if half:
                block.append(jnp.broadcast_to(offset, (SUBLANES, HEAD_DIM)))
            columns.append(jnp.concatenate(block, 0).astype(jnp.bfloat16))
        depth = STRIDE * HEAD_DIM
        halves.append(
            jnp.dot(
                jnp.concatenate(columns, 1),
                weight[half * depth : (half + 1) * depth, :],
                preferred_element_type=jnp.float32,
            )
        )
    first, second = halves
    last = second[heads * blocks : heads * blocks + 1, :]
    result = []
    for head in range(heads):
        start = head * blocks
        after = jnp.concatenate([second[start + 1 : start + blocks, :], last], 0)
        result.append((first[start : start + blocks, :] + after).astype(jnp.bfloat16))
    return result


def attention_kernel(
    k_mine,
    k_other,
    v_mine,
    v_other,
    q_mine,
    q_other,
    position,
    weight_k,
    weight_v,
    visible,
    out,
    k_rows,
    v_rows,
    q_rows,
):
    core = lax.axis_index("seq")
    length, width = k_mine.shape
    heads = width // HEAD_DIM
    strides = length // STRIDE
    for rows, mine, other in ((k_rows, k_mine, k_other), (v_rows, v_mine, v_other)):
        for place, half in ((core, mine), (1 - core, other)):
            where = pl.ds(pl.multiple_of(place * strides, strides), strides)
            for head in range(heads):
                block = half[:, head * HEAD_DIM : (head + 1) * HEAD_DIM].astype(jnp.float32)
                block = block.reshape(strides, STRIDE, HEAD_DIM)
                rows[head, :, where, :] = jnp.swapaxes(block, 0, 1)
    few = q_mine.shape[0]
    mine = q_mine[...].astype(jnp.float32)
    other = q_other[...].astype(jnp.float32)
    q_rows[:few, :] = jnp.where(core == 0, mine, other)
    q_rows[few:, :] = jnp.where(core == 0, other, mine)
    count = 2 * few
    keys = compress_all(k_rows, position, weight_k)
    values = compress_all(v_rows, position, weight_v)
    group = q_rows.shape[1] // HEAD_DIM // heads
    seen = visible[...].reshape(group * count, visible.shape[2]) > 0.0
    lanes = []
    for head in range(heads):
        query = jnp.concatenate(
            [
                q_rows[:, (head * group + g) * HEAD_DIM : (head * group + g + 1) * HEAD_DIM]
                for g in range(group)
            ],
            0,
        ).astype(jnp.bfloat16)
        scores = lax.dot_general(query, keys[head], NT, preferred_element_type=jnp.float32)
        scores = jnp.where(seen, scores * (1.0 / math.sqrt(HEAD_DIM)), -1e30)
        peak = jnp.max(scores, -1, keepdims=True)
        weights = jnp.where(seen, jnp.exp(scores - peak), 0.0)
        probs = (weights / jnp.sum(weights, -1, keepdims=True)).astype(jnp.bfloat16)
        attended = jnp.dot(probs, values[head], preferred_element_type=jnp.float32)
        attended = attended.astype(jnp.bfloat16).astype(jnp.float32)
        lanes += [attended[g * count : (g + 1) * count, :] for g in range(group)]
    out[...] = jnp.concatenate(lanes, 1).astype(jnp.bfloat16)


def product_kernel(attended, out_proj, residual, part):
    mine = residual[lax.axis_index("batch")].astype(jnp.float32)
    part[...] = jnp.where(lax.axis_index("mp") == 0, mine, 0.0) + jnp.dot(
        attended[...], out_proj[...], preferred_element_type=jnp.float32
    )


def visible_kernel(skip, visible):
    row = lax.broadcasted_iota(jnp.int32, visible.shape, 1)
    block = lax.broadcasted_iota(jnp.int32, visible.shape, 2)
    visible[...] = (block <= row * skip // STRIDE).astype(jnp.float32)


def visible_blocks(group, count, blocks, skip):
    return pl.pallas_call(
        functools.partial(visible_kernel, skip),
        out_shape=jax.ShapeDtypeStruct((group, count, blocks), jnp.float32),
        out_specs=VMEM,
        compiler_params=pltpu.CompilerParams(vmem_limit_bytes=4 << 20),
        cost_estimate=pl.CostEstimate(flops=FILL, bytes_accessed=0, transcendentals=0),
        name="visible",
    )()


def attention(keys, values, queries, key_position, compress_keys, compress_values, skip):
    length, width = keys.shape
    heads = width // HEAD_DIM
    count = 2 * queries.shape[0]
    group = queries.shape[1] // HEAD_DIM // heads
    rows = pltpu.VMEM((heads, STRIDE, 2 * length // STRIDE, HEAD_DIM), jnp.float32)
    return pl.pallas_call(
        attention_kernel,
        out_shape=jax.ShapeDtypeStruct((count, queries.shape[1]), jnp.bfloat16),
        in_specs=[VMEM] * 10,
        out_specs=VMEM,
        scratch_shapes=[rows, rows, pltpu.VMEM((count, queries.shape[1]), jnp.float32)],
        compiler_params=pltpu.CompilerParams(vmem_limit_bytes=16 << 20),
        cost_estimate=pl.CostEstimate(
            flops=16 * length * width * HEAD_DIM,
            bytes_accessed=2 * (compress_keys.size + compress_values.size),
            transcendentals=count * 1024,
        ),
        name="attention",
    )(
        keys,
        swap(keys),
        values,
        swap(values),
        queries,
        swap(queries),
        key_position,
        compress_keys,
        compress_values,
        visible_blocks(group, count, 2 * length // STRIDE, skip),
    )


def product(attended, out_proj, residual):
    return pl.pallas_call(
        product_kernel,
        out_shape=jax.ShapeDtypeStruct(residual.shape[1:], jnp.float32),
        in_specs=[VMEM] * 3,
        out_specs=VMEM,
        compiler_params=pltpu.CompilerParams(vmem_limit_bytes=16 << 20),
        cost_estimate=pl.CostEstimate(
            flops=FILL,
            bytes_accessed=2 * out_proj.size,
            transcendentals=0,
        ),
        name="product",
    )(attended, out_proj, residual)


def place_rows(mine, others, scored, rows):
    place = lax.axis_index("batch")
    for distance in range(1 + others.shape[0] // scored):
        start = pl.multiple_of(lax.bitwise_xor(place, distance) * scored, scored)
        if distance:
            block = others[(distance - 1) * scored : distance * scored, :]
        else:
            block = mine[...]
        rows[pl.ds(start, scored), :] = block.astype(jnp.float32)


def near_kernel(scored, mine, others, rows, squares):
    place_rows(mine, others, scored, rows)
    half = rows[...]
    squares[...] = jnp.sum(half * half, -1, keepdims=True)


def near_half(mine, others):
    scored, width = mine.shape
    rows = scored + others.shape[0]
    return pl.pallas_call(
        functools.partial(near_kernel, scored),
        out_shape=(
            jax.ShapeDtypeStruct((rows, width), jnp.float32),
            jax.ShapeDtypeStruct((rows, 1), jnp.float32),
        ),
        in_specs=[VMEM] * 2,
        out_specs=(VMEM, VMEM),
        compiler_params=pltpu.CompilerParams(vmem_limit_bytes=8 << 20),
        cost_estimate=pl.CostEstimate(flops=FILL // 10, bytes_accessed=0, transcendentals=0),
        name="near",
    )(mine, others)


def logits_kernel(scored, skip, *refs):
    near, squares, far_mine, far_others, gain, lm_head, facts, sent, far, both = refs
    core = lax.axis_index("seq")
    width = near.shape[1]
    place_rows(far_mine, far_others, scored, far)
    rest = far[...]
    meansq = (squares[...] + jnp.sum(rest * rest, -1, keepdims=True)) / both.shape[1]
    scale = lax.rsqrt(meansq + 1e-05)
    for side, half in ((core, near[...]), (1 - core, rest)):
        columns = pl.ds(pl.multiple_of(side * width, width), width)
        both[:, columns] = (half * scale * gain[:, columns]).astype(jnp.bfloat16)
    normed = both[...]
    logits = lax.dot_general(lm_head[...], normed, NT, preferred_element_type=jnp.float32)
    share, rows = logits.shape
    offset = device_index() * share
    ids = offset + lax.broadcasted_iota(jnp.int32, (share, rows), 0)
    top = jnp.max(logits, 0, keepdims=True)
    total = jnp.sum(jnp.exp(logits - top), 0, keepdims=True)
    picked = jnp.sum(jnp.where(ids == facts[0:1, :], logits, 0.0), 0, keepdims=True)
    spots = lax.broadcasted_iota(jnp.int32, (1, rows), 1) % scored * skip + BLOCK - 1
    valid = (spots < facts[1:2, :]).astype(jnp.float32)
    known = [top, total, picked, valid]
    if sent.shape[1] > 4 * rows:
        known.append(jnp.zeros((1, sent.shape[1] - 4 * rows), jnp.float32))
    sent[...] = jnp.broadcast_to(jnp.concatenate(known, 1), sent.shape)


def device_index():
    index = 0
    for axis in EVERY:
        index = index * lax.axis_size(axis) + lax.axis_index(axis)
    return index


def share_statistics(near, far, norm_gain, lm_head, targets, lengths, skip):
    scored = targets.shape[1]
    facts = jnp.stack([targets.reshape(-1), jnp.repeat(lengths, scored)], 0)
    rows = facts.shape[1]
    across = -(-4 * rows // LANES) * LANES
    return pl.pallas_call(
        functools.partial(logits_kernel, scored, skip),
        out_shape=jax.ShapeDtypeStruct((lax.axis_size(EVERY), across), jnp.float32),
        in_specs=[VMEM] * (2 * len(near) + 3),
        out_specs=VMEM,
        scratch_shapes=[
            pltpu.VMEM((rows, far[0].shape[1]), jnp.float32),
            pltpu.VMEM((rows, lm_head.shape[1]), jnp.bfloat16),
        ],
        compiler_params=pltpu.CompilerParams(vmem_limit_bytes=16 << 20),
        cost_estimate=pl.CostEstimate(
            flops=2 * rows * lm_head.size, bytes_accessed=2 * lm_head.size, transcendentals=rows * 1024
        ),
        name="statistics",
    )(*near, *far, norm_gain.reshape(1, -1), lm_head, facts)


def score_kernel(rows, scored, few, got, token, score):
    tops = got[:, :rows]
    top = jnp.max(tops, 0, keepdims=True)
    total = jnp.sum(got[:, rows : 2 * rows] * jnp.exp(tops - top), 0, keepdims=True)
    picked = jnp.sum(got[:, 2 * rows : 3 * rows], 0, keepdims=True)
    logprob = picked - (top + jnp.log(total))
    index = lax.broadcasted_iota(jnp.int32, (1, rows), 1)
    valid = got[0:1, 3 * rows : 4 * rows]
    count = jnp.sum(valid, 1, keepdims=True)
    batch = lax.axis_index("batch")
    mine = jnp.where(index // scored == batch, valid * logprob, 0.0)
    score[...] = jnp.sum(mine, 1, keepdims=True) / count
    start = batch * scored + lax.axis_index("seq") * few
    spare = jnp.zeros((1, got.shape[1] - rows), jnp.float32)
    turned = pltpu.roll(
        jnp.concatenate([logprob, spare], 1), lax.rem(got.shape[1] - start, got.shape[1]), 1
    )
    token[...] = turned[:, :few]


def final_scores(got, rows, scored, few):
    token, score = pl.pallas_call(
        functools.partial(score_kernel, rows, scored, few),
        out_shape=(
            jax.ShapeDtypeStruct((1, few), jnp.float32),
            jax.ShapeDtypeStruct((1, 1), jnp.float32),
        ),
        in_specs=[VMEM],
        out_specs=(VMEM, VMEM),
        compiler_params=pltpu.CompilerParams(vmem_limit_bytes=4 << 20),
        name="scores",
    )(got)
    return token, score.reshape(1)


def small_mesh(
    queries,
    keys,
    values,
    key_position,
    compress_keys,
    compress_values,
    out_proj,
    residual,
    norm_gain,
    lm_head,
    targets,
    lengths,
):
    few = queries.shape[1]
    skip = keys.shape[1] // few
    attended = attention(
        keys[0], values[0], queries[0], key_position, compress_keys, compress_values, skip
    )
    part = product(attended, out_proj, residual)
    parts = [swap(part)]
    parts += crossed_all(part, "mp")
    far = [pair_sum(parts).astype(jnp.bfloat16)]
    near = crossed_all(far[0], "batch")
    near = [swap(far[0]), jnp.concatenate(near, 0)]
    far.append(swap(near[1]))
    near = near_half(*near)
    sent = share_statistics(near, far, norm_gain, lm_head, targets, lengths, skip)
    got = lax.all_to_all(sent, EVERY, 0, 0, tiled=True)
    return final_scores(got, targets.size, targets.shape[1], few)


def body(*arrays):
    small = (
        lax.axis_size("seq") == 2
        and direct("mp")
        and direct("batch")
        and lax.axis_size(EVERY) <= SPREAD
    )
    return small_mesh(*arrays) if small else large_mesh(*arrays)


def solution(mesh):
    in_specs = (
        P("batch", "seq", "mp"),
        P("batch", "seq", "mp"),
        P("batch", "seq", "mp"),
        P(),
        P(),
        P(),
        P("mp", "seq"),
        P(None, None, "seq"),
        P(),
        P(("seq", "mp", "batch"), None),
        P(),
        P(),
    )
    out_specs = (P("batch", "seq"), P("batch"))
    return jax.shard_map(body, mesh=mesh, in_specs=in_specs, out_specs=out_specs, check_vma=False)
```

```python
import functools
import math

import jax
import jax.numpy as jnp
from jax import lax
from jax.experimental import pallas as pl
from jax.experimental.pallas import tpu as pltpu
from jax.sharding import PartitionSpec as P


HEAD_DIM = 128
BLOCK = 32
STRIDE = 16


def from_behind(block, axis, distance):
    devices = range(lax.axis_size(axis))
    route = [(i - distance, i) for i in devices if i - distance in devices]
    return lax.ppermute(block, axis, route)


def compress_rows(rows, following, position, weight):
    extended = jnp.concatenate([rows, following], 0)
    count = rows.shape[0] // STRIDE
    heads = rows.shape[1] // HEAD_DIM
    shaped = extended.reshape(count + 1, STRIDE, heads, HEAD_DIM)
    blocks = jnp.concatenate([shaped[:-1], shaped[1:]], 1)
    blocks = (blocks.astype(jnp.float32) + position[None, :, None, :]).astype(jnp.bfloat16)
    mapped = jnp.einsum(
        "bjhd,jde->bhe",
        blocks,
        weight.reshape(BLOCK, HEAD_DIM, HEAD_DIM),
        preferred_element_type=jnp.float32,
    )
    return mapped.astype(jnp.bfloat16).reshape(count, heads * HEAD_DIM)


def normalize(hidden, gain):
    widened = hidden.astype(jnp.float32)
    meansq = jnp.mean(widened * widened, -1, keepdims=True)
    return (widened * lax.rsqrt(meansq + 1e-05) * gain).astype(jnp.bfloat16)


def vocab_logits(normed, rows):
    return lax.dot_general(
        normed, rows, (((1,), (1,)), ((), ())), preferred_element_type=jnp.float32
    )


def picked_logit(logits, offset, wanted):
    columns = offset + jnp.arange(logits.shape[1], dtype=jnp.int32)
    hits = columns[None, :] == wanted[:, None]
    return jnp.sum(jnp.where(hits, logits, 0.0), 1)


DIRECT = 4
SPREAD = 64


def pairs(axis, distance):
    return [(i, i ^ distance) for i in range(lax.axis_size(axis))]


def direct(axis):
    count = lax.axis_size(axis)
    return count <= DIRECT and count & (count - 1) == 0


def exchange(block, axis):
    return [block] + [
        lax.ppermute(block, axis, pairs(axis, distance))
        for distance in range(1, lax.axis_size(axis))
    ]


def by_position(blocks, axis):
    place = lax.axis_index(axis)
    step = 1
    while step < len(blocks):
        odd = (place // step) % 2 == 1
        blocks = [jnp.where(odd, blocks[i ^ step], blocks[i]) for i in range(len(blocks))]
        step *= 2
    return blocks


def pair_sum(blocks):
    while len(blocks) > 1:
        blocks = [blocks[i] + blocks[i + 1] for i in range(0, len(blocks), 2)]
    return blocks[0]


def sum_over(part, axis):
    if direct(axis):
        return pair_sum(exchange(part, axis))
    return lax.psum(part, axis)


def gather_over(block, axis, dimension):
    if direct(axis):
        return jnp.concatenate(by_position(exchange(block, axis), axis), dimension)
    return lax.all_gather(block, axis, axis=dimension, tiled=True)


def attend(query, all_keys, all_values, first, skip):
    count = query.shape[0]
    blocks = all_keys.shape[0]
    scores = jnp.einsum("qhgd,bhd->qhgb", query, all_keys, preferred_element_type=jnp.float32) * (
        1.0 / math.sqrt(HEAD_DIM)
    )
    index = first + jnp.arange(count, dtype=jnp.int32)
    limit = index * skip // STRIDE
    visible = (jnp.arange(blocks, dtype=jnp.int32)[None, :] <= limit[:, None])[:, None, None, :]
    scores = jnp.where(visible, scores, -1e30)
    peak = jnp.max(scores, -1, keepdims=True)
    weights = jnp.where(visible, jnp.exp(scores - peak), 0.0)
    probs = (weights / jnp.sum(weights, -1, keepdims=True)).astype(jnp.bfloat16)
    attended = jnp.einsum("qhgb,bhd->qhgd", probs, all_values, preferred_element_type=jnp.float32)
    return attended.astype(jnp.bfloat16).reshape(count, -1)


def attend_whole(queries, keys, values, key_position, compress_keys, compress_values, skip):
    rows = gather_over(keys, "seq", 0)
    vals = gather_over(values, "seq", 0)
    query = gather_over(queries, "seq", 0)
    none = jnp.zeros((STRIDE, rows.shape[1]), rows.dtype)
    comp_keys = compress_rows(rows, none, key_position, compress_keys)
    comp_values = compress_rows(vals, none, key_position, compress_values)
    heads = rows.shape[1] // HEAD_DIM
    group = query.shape[1] // HEAD_DIM // heads
    return attend(
        query.reshape(-1, heads, group, HEAD_DIM),
        comp_keys.reshape(-1, heads, HEAD_DIM),
        comp_values.reshape(-1, heads, HEAD_DIM),
        0,
        skip,
    )


def attend_segments(queries, keys, values, key_position, compress_keys, compress_values, skip):
    following = from_behind((keys[:STRIDE], values[:STRIDE]), "seq", -1)
    comp_keys = compress_rows(keys, following[0], key_position, compress_keys)
    comp_values = compress_rows(values, following[1], key_position, compress_values)
    every = lax.all_gather(jnp.stack([comp_keys, comp_values], 0), "seq", axis=1, tiled=True)
    heads = keys.shape[1] // HEAD_DIM
    group = queries.shape[1] // HEAD_DIM // heads
    blocks = every.shape[1]
    attended = attend(
        queries.reshape(-1, heads, group, HEAD_DIM),
        every[0].reshape(blocks, heads, HEAD_DIM),
        every[1].reshape(blocks, heads, HEAD_DIM),
        lax.axis_index("seq") * queries.shape[0],
        skip,
    )
    return lax.all_gather(attended, "seq", axis=0, tiled=True)


EVERY = ("seq", "mp", "batch")


def log_probs(logits, wanted, offset):
    picked = picked_logit(logits, offset, wanted)
    local_top = jnp.max(logits, 1)
    devices = lax.axis_size(EVERY)
    if devices > SPREAD:
        top = lax.pmax(local_top, EVERY)
        local_sum = jnp.sum(jnp.exp(logits - top[:, None]), 1)
        total, target_logit = lax.psum((local_sum, picked), EVERY)
        return target_logit - (top + jnp.log(total))
    local_sum = jnp.sum(jnp.exp(logits - local_top[:, None]), 1)
    mine = jnp.concatenate([local_top, local_sum, picked], 0)
    sent = jnp.broadcast_to(mine[None, :], (devices, mine.shape[0]))
    tops, sums, hits = jnp.split(lax.all_to_all(sent, EVERY, 0, 0, tiled=True), 3, 1)
    top = jnp.max(tops, 0)
    total = jnp.sum(sums * jnp.exp(tops - top[None, :]), 0)
    return jnp.sum(hits, 0) - (top + jnp.log(total))


def large_mesh(
    queries,
    keys,
    values,
    key_position,
    compress_keys,
    compress_values,
    out_proj,
    residual,
    norm_gain,
    lm_head,
    targets,
    lengths,
):
    seq_pos = lax.axis_index("seq")
    batch_pos = lax.axis_index("batch")
    qcount = queries.shape[1]
    skip = keys.shape[1] // qcount
    rollouts, scored = targets.shape
    attending = attend_whole if direct("seq") else attend_segments
    attended = attending(
        queries[0], keys[0], values[0], key_position, compress_keys, compress_values, skip
    )
    part = jnp.dot(attended, out_proj, preferred_element_type=jnp.float32)
    summed = sum_over(part, "mp")
    hidden = (residual[batch_pos].astype(jnp.float32) + summed).astype(jnp.bfloat16)
    whole = gather_over(gather_over(hidden, "batch", 0), "seq", 1)
    normed = normalize(whole, norm_gain)
    logits = vocab_logits(normed, lm_head)
    offset = lax.axis_index(EVERY) * lm_head.shape[0]
    by_rollout = log_probs(logits, targets.reshape(-1), offset).reshape(rollouts, scored)
    spots = jnp.arange(scored, dtype=jnp.int32) * skip + BLOCK - 1
    valid = (spots[None, :] < lengths[:, None]).astype(jnp.float32)
    count = jnp.sum(valid)
    token_logprob = lax.dynamic_slice(by_rollout, (batch_pos, seq_pos * qcount), (1, qcount))
    sums = jnp.sum(valid * by_rollout, 1) / count
    rollout_score = sums[batch_pos][None]
    return (token_logprob, rollout_score)


VMEM = pl.BlockSpec(memory_space=pltpu.VMEM)
SMEM = pl.BlockSpec(memory_space=pltpu.SMEM)
NT = (((1,), (1,)), ((), ()))
LANES = 128
SUBLANES = 8
FILL = 20_000_000_000


def swap(block):
    return lax.ppermute(block, "seq", [(0, 1), (1, 0)])


def crossed(block, axis, distance):
    count = lax.axis_size(axis)
    route = [
        (core * count + i, (1 - core) * count + (i ^ distance))
        for core in range(2)
        for i in range(count)
    ]
    return lax.ppermute(block, ("seq", axis), route)


def crossed_all(block, axis):
    return [crossed(block, axis, d) for d in range(lax.axis_size(axis) - 1, 0, -1)][::-1]


def compress_all(rows, position, weight):
    heads, _, blocks, _ = rows.shape
    halves = []
    for half in range(BLOCK // STRIDE):
        columns = []
        for i in range(STRIDE):
            offset = position[half * STRIDE + i : half * STRIDE + i + 1, :]
            block = [rows[head, i] + offset for head in range(heads)]
            if half:
                block.append(jnp.broadcast_to(offset, (SUBLANES, HEAD_DIM)))
            columns.append(jnp.concatenate(block, 0).astype(jnp.bfloat16))
        depth = STRIDE * HEAD_DIM
        halves.append(
            jnp.dot(
                jnp.concatenate(columns, 1),
                weight[half * depth : (half + 1) * depth, :],
                preferred_element_type=jnp.float32,
            )
        )
    first, second = halves
    last = second[heads * blocks : heads * blocks + 1, :]
    result = []
    for head in range(heads):
        start = head * blocks
        after = jnp.concatenate([second[start + 1 : start + blocks, :], last], 0)
        result.append((first[start : start + blocks, :] + after).astype(jnp.bfloat16))
    return result


def attention_kernel(
    k_mine,
    k_other,
    v_mine,
    v_other,
    q_mine,
    q_other,
    position,
    weight_k,
    weight_v,
    visible,
    out,
    k_rows,
    v_rows,
    q_rows,
):
    core = lax.axis_index("seq")
    length, width = k_mine.shape
    heads = width // HEAD_DIM
    strides = length // STRIDE
    for rows, mine, other in ((k_rows, k_mine, k_other), (v_rows, v_mine, v_other)):
        for place, half in ((core, mine), (1 - core, other)):
            where = pl.ds(pl.multiple_of(place * strides, strides), strides)
            for head in range(heads):
                block = half[:, head * HEAD_DIM : (head + 1) * HEAD_DIM].astype(jnp.float32)
                block = block.reshape(strides, STRIDE, HEAD_DIM)
                rows[head, :, where, :] = jnp.swapaxes(block, 0, 1)
    few = q_mine.shape[0]
    mine = q_mine[...].astype(jnp.float32)
    other = q_other[...].astype(jnp.float32)
    q_rows[:few, :] = jnp.where(core == 0, mine, other)
    q_rows[few:, :] = jnp.where(core == 0, other, mine)
    count = 2 * few
    keys = compress_all(k_rows, position, weight_k)
    values = compress_all(v_rows, position, weight_v)
    group = q_rows.shape[1] // HEAD_DIM // heads
    seen = visible[...].reshape(group * count, visible.shape[2]) > 0.0
    lanes = []
    for head in range(heads):
        query = jnp.concatenate(
            [
                q_rows[:, (head * group + g) * HEAD_DIM : (head * group + g + 1) * HEAD_DIM]
                for g in range(group)
            ],
            0,
        ).astype(jnp.bfloat16)
        scores = lax.dot_general(query, keys[head], NT, preferred_element_type=jnp.float32)
        scores = jnp.where(seen, scores * (1.0 / math.sqrt(HEAD_DIM)), -1e30)
        peak = jnp.max(scores, -1, keepdims=True)
        weights = jnp.where(seen, jnp.exp(scores - peak), 0.0)
        probs = (weights / jnp.sum(weights, -1, keepdims=True)).astype(jnp.bfloat16)
        attended = jnp.dot(probs, values[head], preferred_element_type=jnp.float32)
        attended = attended.astype(jnp.bfloat16).astype(jnp.float32)
        lanes += [attended[g * count : (g + 1) * count, :] for g in range(group)]
    out[...] = jnp.concatenate(lanes, 1).astype(jnp.bfloat16)


def product_kernel(attended, out_proj, residual, part):
    mine = residual[lax.axis_index("batch")].astype(jnp.float32)
    part[...] = jnp.where(lax.axis_index("mp") == 0, mine, 0.0) + jnp.dot(
        attended[...], out_proj[...], preferred_element_type=jnp.float32
    )


def visible_kernel(skip, visible):
    row = lax.broadcasted_iota(jnp.int32, visible.shape, 1)
    block = lax.broadcasted_iota(jnp.int32, visible.shape, 2)
    visible[...] = (block <= row * skip // STRIDE).astype(jnp.float32)


def visible_blocks(group, count, blocks, skip):
    return pl.pallas_call(
        functools.partial(visible_kernel, skip),
        out_shape=jax.ShapeDtypeStruct((group, count, blocks), jnp.float32),
        out_specs=VMEM,
        compiler_params=pltpu.CompilerParams(vmem_limit_bytes=4 << 20),
        cost_estimate=pl.CostEstimate(flops=FILL, bytes_accessed=0, transcendentals=0),
        name="visible",
    )()


def attention(keys, values, queries, key_position, compress_keys, compress_values, skip):
    length, width = keys.shape
    heads = width // HEAD_DIM
    count = 2 * queries.shape[0]
    group = queries.shape[1] // HEAD_DIM // heads
    rows = pltpu.VMEM((heads, STRIDE, 2 * length // STRIDE, HEAD_DIM), jnp.float32)
    return pl.pallas_call(
        attention_kernel,
        out_shape=jax.ShapeDtypeStruct((count, queries.shape[1]), jnp.bfloat16),
        in_specs=[VMEM] * 10,
        out_specs=VMEM,
        scratch_shapes=[rows, rows, pltpu.VMEM((count, queries.shape[1]), jnp.float32)],
        compiler_params=pltpu.CompilerParams(vmem_limit_bytes=16 << 20),
        cost_estimate=pl.CostEstimate(
            flops=16 * length * width * HEAD_DIM,
            bytes_accessed=2 * (compress_keys.size + compress_values.size),
            transcendentals=count * 1024,
        ),
        name="attention",
    )(
        keys,
        swap(keys),
        values,
        swap(values),
        queries,
        swap(queries),
        key_position,
        compress_keys,
        compress_values,
        visible_blocks(group, count, 2 * length // STRIDE, skip),
    )


def product(attended, out_proj, residual):
    return pl.pallas_call(
        product_kernel,
        out_shape=jax.ShapeDtypeStruct(residual.shape[1:], jnp.float32),
        in_specs=[VMEM] * 3,
        out_specs=VMEM,
        compiler_params=pltpu.CompilerParams(vmem_limit_bytes=16 << 20),
        cost_estimate=pl.CostEstimate(
            flops=FILL,
            bytes_accessed=2 * out_proj.size,
            transcendentals=0,
        ),
        name="product",
    )(attended, out_proj, residual)


def logits_kernel(scored, skip, *refs):
    near_mine, near_others, far_mine, far_others, gain, lm_head, facts, sent, hidden = refs
    core = lax.axis_index("seq")
    place = lax.axis_index("batch")
    width = near_mine.shape[1]
    for side, mine, others in ((core, near_mine, near_others), (1 - core, far_mine, far_others)):
        columns = pl.ds(pl.multiple_of(side * width, width), width)
        for distance in range(1 + others.shape[0] // scored):
            start = pl.multiple_of(lax.bitwise_xor(place, distance) * scored, scored)
            if distance:
                block = others[(distance - 1) * scored : distance * scored, :]
            else:
                block = mine[...]
            hidden[pl.ds(start, scored), columns] = block.astype(jnp.float32)
    whole = hidden[...]
    meansq = jnp.mean(whole * whole, -1, keepdims=True)
    normed = (whole * lax.rsqrt(meansq + 1e-05) * gain[...]).astype(jnp.bfloat16)
    logits = lax.dot_general(lm_head[...], normed, NT, preferred_element_type=jnp.float32)
    share, rows = logits.shape
    offset = device_index() * share
    ids = offset + lax.broadcasted_iota(jnp.int32, (share, rows), 0)
    top = jnp.max(logits, 0, keepdims=True)
    total = jnp.sum(jnp.exp(logits - top), 0, keepdims=True)
    picked = jnp.sum(jnp.where(ids == facts[0:1, :], logits, 0.0), 0, keepdims=True)
    spots = lax.broadcasted_iota(jnp.int32, (1, rows), 1) % scored * skip + BLOCK - 1
    valid = (spots < facts[1:2, :]).astype(jnp.float32)
    known = [top, total, picked, valid]
    if sent.shape[1] > 4 * rows:
        known.append(jnp.zeros((1, sent.shape[1] - 4 * rows), jnp.float32))
    sent[...] = jnp.broadcast_to(jnp.concatenate(known, 1), sent.shape)


def device_index():
    index = 0
    for axis in EVERY:
        index = index * lax.axis_size(axis) + lax.axis_index(axis)
    return index


def share_statistics(near, far, norm_gain, lm_head, targets, lengths, skip):
    scored = targets.shape[1]
    facts = jnp.stack([targets.reshape(-1), jnp.repeat(lengths, scored)], 0)
    rows = facts.shape[1]
    across = -(-4 * rows // LANES) * LANES
    return pl.pallas_call(
        functools.partial(logits_kernel, scored, skip),
        out_shape=jax.ShapeDtypeStruct((lax.axis_size(EVERY), across), jnp.float32),
        in_specs=[VMEM] * (2 * len(near) + 3),
        out_specs=VMEM,
        scratch_shapes=[pltpu.VMEM((rows, lm_head.shape[1]), jnp.float32)],
        compiler_params=pltpu.CompilerParams(vmem_limit_bytes=16 << 20),
        cost_estimate=pl.CostEstimate(
            flops=2 * rows * lm_head.size, bytes_accessed=2 * lm_head.size, transcendentals=rows * 1024
        ),
        name="statistics",
    )(*near, *far, norm_gain.reshape(1, -1), lm_head, facts)


def score_kernel(rows, scored, few, got, token, score):
    tops = got[:, :rows]
    top = jnp.max(tops, 0, keepdims=True)
    total = jnp.sum(got[:, rows : 2 * rows] * jnp.exp(tops - top), 0, keepdims=True)
    picked = jnp.sum(got[:, 2 * rows : 3 * rows], 0, keepdims=True)
    logprob = picked - (top + jnp.log(total))
    index = lax.broadcasted_iota(jnp.int32, (1, rows), 1)
    valid = got[0:1, 3 * rows : 4 * rows]
    count = jnp.sum(valid, 1, keepdims=True)
    batch = lax.axis_index("batch")
    mine = jnp.where(index // scored == batch, valid * logprob, 0.0)
    score[...] = jnp.sum(mine, 1, keepdims=True) / count
    start = batch * scored + lax.axis_index("seq") * few
    spare = jnp.zeros((1, got.shape[1] - rows), jnp.float32)
    turned = pltpu.roll(
        jnp.concatenate([logprob, spare], 1), lax.rem(got.shape[1] - start, got.shape[1]), 1
    )
    token[...] = turned[:, :few]


def final_scores(got, rows, scored, few):
    token, score = pl.pallas_call(
        functools.partial(score_kernel, rows, scored, few),
        out_shape=(
            jax.ShapeDtypeStruct((1, few), jnp.float32),
            jax.ShapeDtypeStruct((1, 1), jnp.float32),
        ),
        in_specs=[VMEM],
        out_specs=(VMEM, VMEM),
        compiler_params=pltpu.CompilerParams(vmem_limit_bytes=4 << 20),
        name="scores",
    )(got)
    return token, score.reshape(1)


def small_mesh(
    queries,
    keys,
    values,
    key_position,
    compress_keys,
    compress_values,
    out_proj,
    residual,
    norm_gain,
    lm_head,
    targets,
    lengths,
):
    few = queries.shape[1]
    skip = keys.shape[1] // few
    attended = attention(
        keys[0], values[0], queries[0], key_position, compress_keys, compress_values, skip
    )
    part = product(attended, out_proj, residual)
    parts = [swap(part)]
    parts += crossed_all(part, "mp")
    far = [pair_sum(parts).astype(jnp.bfloat16)]
    near = crossed_all(far[0], "batch")
    near = [swap(far[0]), jnp.concatenate(near, 0)]
    far.append(swap(near[1]))
    sent = share_statistics(near, far, norm_gain, lm_head, targets, lengths, skip)
    got = lax.all_to_all(sent, EVERY, 0, 0, tiled=True)
    return final_scores(got, targets.size, targets.shape[1], few)


def body(*arrays):
    small = (
        lax.axis_size("seq") == 2
        and direct("mp")
        and direct("batch")
        and lax.axis_size(EVERY) <= SPREAD
    )
    return small_mesh(*arrays) if small else large_mesh(*arrays)


def solution(mesh):
    in_specs = (
        P("batch", "seq", "mp"),
        P("batch", "seq", "mp"),
        P("batch", "seq", "mp"),
        P(),
        P(),
        P(),
        P("mp", "seq"),
        P(None, None, "seq"),
        P(),
        P(("seq", "mp", "batch"), None),
        P(),
        P(),
    )
    out_specs = (P("batch", "seq"), P("batch"))
    return jax.shard_map(body, mesh=mesh, in_specs=in_specs, out_specs=out_specs, check_vma=False)
```
